16 devices in a mesh: dp: 2 (over y, z), sp: 8 (over x, core).
Axes of the slice: x: 4, y: 2, z: 1, core: 2. Of those that a mesh axis runs over, the one named last changes fastest.
The devices are a block of a 4x4x8 slice.
Arguments:
- latent: bfloat16 [24, 64, 16, 640], P('dp', 'sp'), parts along dimension 0
- context: bfloat16 [24, 77, 2048], P('dp'), parts along dimension 0
- gn_gain: bfloat16 [640], replicated
- gn_bias: bfloat16 [640], replicated
- w_in: bfloat16 [640, 640], replicated
- b_in: bfloat16 [640], replicated
- ln_gain: bfloat16 [2, 3, 640], replicated
- ln_bias: bfloat16 [2, 3, 640], replicated
- w_self: bfloat16 [2, 4, 640, 640], replicated
- b_self: bfloat16 [2, 640], replicated
- w_cross_q: bfloat16 [2, 640, 640], replicated
- w_cross_kv: bfloat16 [2, 2, 2048, 640], replicated
- w_cross_o: bfloat16 [2, 640, 640], replicated
- b_cross: bfloat16 [2, 640], replicated
- w_ff1: bfloat16 [2, 640, 5120], replicated
- b_ff1: bfloat16 [2, 5120], replicated
- w_ff2: bfloat16 [2, 2560, 640], replicated
- b_ff2: bfloat16 [2, 640], replicated
- w_out: bfloat16 [640, 640], replicated
- b_out: bfloat16 [640], replicated
Outputs:
- output: bfloat16 [24, 64, 16, 640], P('dp', 'sp'), parts along dimension 0
There are 2 independent parts. The reference program is written for one: setup_inputs(seed, part) draws one part's arguments, and reference() takes and returns one part's arrays. A program takes and returns all parts, laid end to end along the dimension named above; an argument that names none is the same for every part.
All inputs are finite; a program needn't handle non-finite values.
Results may differ from the reference program's by a relative error of at most 0.0130236.
Values are sent between devices in bfloat16 or wider.
A program may use at most 768 MiB of HBM per device.

```python
import jax
import jax.numpy as jnp
from jax import lax

BATCH_SIZE = 12
LAT_ROWS = 64
LAT_COLS = 16
CHANNELS = 640
NUM_HEADS = 10
HEAD_DIM = 64
TEXT_LEN = 77
TEXT_DIM = 2048
FF_DIM = 2560
NUM_GROUPS = 32
NUM_LAYERS = 2


def draw_normal(key, shape, scale):
    return jax.random.normal(key, shape, jnp.float32) * scale


def setup_inputs(seed: int = 0, part: int = 0) -> dict:
    part_key = jax.random.fold_in(jax.random.key(seed), part)
    lat_keys = jax.random.split(part_key, 8)
    weight_keys = jax.random.split(jax.random.key(seed + 1), 20)
    group_ch = CHANNELS // NUM_GROUPS
    row_pos = (jnp.arange(LAT_ROWS, dtype=jnp.float32) + 0.5) / LAT_ROWS
    basis = jnp.cos(jnp.pi * row_pos[:, None] * jnp.arange(4, dtype=jnp.float32)[None, :])
    group_coef = draw_normal(lat_keys[0], (BATCH_SIZE, 4, NUM_GROUPS, 1), 1.0)
    chan_coef = draw_normal(lat_keys[1], (BATCH_SIZE, 4, NUM_GROUPS, group_ch), 0.5)
    mix_coef = (group_coef + chan_coef).reshape(BATCH_SIZE, 4, CHANNELS)
    row_mean = 0.7 * jnp.einsum('rk,bkc->brc', basis, mix_coef)
    scale_coef = draw_normal(lat_keys[2], (BATCH_SIZE, 4), 1.0)
    row_scale = jnp.exp(0.5 * jnp.einsum('rk,bk->br', basis, scale_coef))
    noise_vals = draw_normal(lat_keys[3], (BATCH_SIZE, LAT_ROWS, LAT_COLS, CHANNELS), 1.0)
    latent = row_mean[:, :, None, :] + row_scale[:, :, None, None] * noise_vals
    context = draw_normal(lat_keys[4], (BATCH_SIZE, 1, TEXT_DIM), 0.8) + draw_normal(lat_keys[5], (BATCH_SIZE, TEXT_LEN, TEXT_DIM), 1.0)
    chan_scale = CHANNELS ** -0.5
    out_boost = jnp.array([1.0, 1.0, 1.0, 2.0], jnp.float32).reshape(1, 4, 1, 1)
    arrays = {
        'latent': latent,
        'context': context,
        'gn_gain': 1.0 + draw_normal(weight_keys[0], (CHANNELS,), 0.3),
        'gn_bias': draw_normal(weight_keys[1], (CHANNELS,), 0.5),
        'w_in': draw_normal(weight_keys[2], (CHANNELS, CHANNELS), chan_scale),
        'b_in': draw_normal(weight_keys[3], (CHANNELS,), 0.5),
        'ln_gain': 1.0 + draw_normal(weight_keys[4], (NUM_LAYERS, 3, CHANNELS), 0.3),
        'ln_bias': draw_normal(weight_keys[5], (NUM_LAYERS, 3, CHANNELS), 0.3),
        'w_self': draw_normal(weight_keys[6], (NUM_LAYERS, 4, CHANNELS, CHANNELS), chan_scale) * out_boost,
        'b_self': draw_normal(weight_keys[7], (NUM_LAYERS, CHANNELS), 0.5),
        'w_cross_q': draw_normal(weight_keys[8], (NUM_LAYERS, CHANNELS, CHANNELS), chan_scale),
        'w_cross_kv': draw_normal(weight_keys[9], (NUM_LAYERS, 2, TEXT_DIM, CHANNELS), TEXT_DIM ** -0.5),
        'w_cross_o': draw_normal(weight_keys[10], (NUM_LAYERS, CHANNELS, CHANNELS), chan_scale),
        'b_cross': draw_normal(weight_keys[11], (NUM_LAYERS, CHANNELS), 0.5),
        'w_ff1': draw_normal(weight_keys[12], (NUM_LAYERS, CHANNELS, 2 * FF_DIM), chan_scale),
        'b_ff1': draw_normal(weight_keys[13], (NUM_LAYERS, 2 * FF_DIM), 0.5),
        'w_ff2': draw_normal(weight_keys[14], (NUM_LAYERS, FF_DIM, CHANNELS), FF_DIM ** -0.5),
        'b_ff2': draw_normal(weight_keys[15], (NUM_LAYERS, CHANNELS), 0.5),
        'w_out': draw_normal(weight_keys[16], (CHANNELS, CHANNELS), chan_scale),
        'b_out': draw_normal(weight_keys[17], (CHANNELS,), 0.5),
    }
    return {name: vals.astype(jnp.bfloat16) for name, vals in arrays.items()}


def layer_norm(hidden, gain, bias):
    vals = hidden.astype(jnp.float32)
    mean_val = jnp.mean(vals, axis=-1, keepdims=True)
    centered = vals - mean_val
    var_val = jnp.mean(centered * centered, axis=-1, keepdims=True)
    scaled = centered * lax.rsqrt(var_val + 1e-5)
    return (scaled * gain.astype(jnp.float32) + bias.astype(jnp.float32)).astype(jnp.bfloat16)


def project(act, weight):
    return jnp.dot(act, weight, preferred_element_type=jnp.float32)


def attend(query, keys, values):
    q_len = query.shape[0]
    k_len = keys.shape[0]
    q_heads = query.reshape(q_len, NUM_HEADS, HEAD_DIM).transpose(1, 0, 2)
    k_heads = keys.reshape(k_len, NUM_HEADS, HEAD_DIM).transpose(1, 0, 2)
    v_heads = values.reshape(k_len, NUM_HEADS, HEAD_DIM).transpose(1, 0, 2)

    def one_head(operands):
        q_one, k_one, v_one = operands
        scores = jnp.dot(q_one, k_one.T, preferred_element_type=jnp.float32) * (HEAD_DIM ** -0.5)
        attn_prob = jax.nn.softmax(scores, axis=-1).astype(jnp.bfloat16)
        return jnp.dot(attn_prob, v_one, preferred_element_type=jnp.float32).astype(jnp.bfloat16)

    head_out = lax.map(one_head, (q_heads, k_heads, v_heads))
    return head_out.transpose(1, 0, 2).reshape(q_len, NUM_HEADS * HEAD_DIM)


def reference(latent, context, gn_gain, gn_bias, w_in, b_in, ln_gain, ln_bias, w_self, b_self, w_cross_q, w_cross_kv, w_cross_o, b_cross, w_ff1, b_ff1, w_ff2, b_ff2, w_out, b_out):
    tokens = LAT_ROWS * LAT_COLS
    group_ch = CHANNELS // NUM_GROUPS

    def one_sample(operands):
        lat_one, ctx_one = operands
        lat_f32 = lat_one.astype(jnp.float32).reshape(tokens, NUM_GROUPS, group_ch)
        grp_mean = jnp.mean(lat_f32, axis=(0, 2), keepdims=True)
        centered = lat_f32 - grp_mean
        grp_var = jnp.mean(centered * centered, axis=(0, 2), keepdims=True)
        normed = (centered * lax.rsqrt(grp_var + 1e-6)).reshape(tokens, CHANNELS)
        normed = (normed * gn_gain.astype(jnp.float32) + gn_bias.astype(jnp.float32)).astype(jnp.bfloat16)
        hidden = (project(normed, w_in) + b_in.astype(jnp.float32)).astype(jnp.bfloat16)

        def block(hidden, layer_w):
            norm_gain, norm_bias, self_w, self_b, cross_q, cross_kv, cross_o, cross_b, ff_in, ff_in_bias, ff_outw, ff_out_bias = layer_w
            normed = layer_norm(hidden, norm_gain[0], norm_bias[0])
            query = project(normed, self_w[0]).astype(jnp.bfloat16)
            keys = project(normed, self_w[1]).astype(jnp.bfloat16)
            values = project(normed, self_w[2]).astype(jnp.bfloat16)
            attn_out = attend(query, keys, values)
            hidden = (hidden.astype(jnp.float32) + project(attn_out, self_w[3]) + self_b.astype(jnp.float32)).astype(jnp.bfloat16)
            normed = layer_norm(hidden, norm_gain[1], norm_bias[1])
            query = project(normed, cross_q).astype(jnp.bfloat16)
            keys = project(ctx_one, cross_kv[0]).astype(jnp.bfloat16)
            values = project(ctx_one, cross_kv[1]).astype(jnp.bfloat16)
            attn_out = attend(query, keys, values)
            hidden = (hidden.astype(jnp.float32) + project(attn_out, cross_o) + cross_b.astype(jnp.float32)).astype(jnp.bfloat16)
            normed = layer_norm(hidden, norm_gain[2], norm_bias[2])
            ff_proj = (project(normed, ff_in) + ff_in_bias.astype(jnp.float32)).astype(jnp.bfloat16)
            gated = (ff_proj[:, :FF_DIM].astype(jnp.float32) * jax.nn.gelu(ff_proj[:, FF_DIM:].astype(jnp.float32), approximate=False)).astype(jnp.bfloat16)
            hidden = (hidden.astype(jnp.float32) + project(gated, ff_outw) + ff_out_bias.astype(jnp.float32)).astype(jnp.bfloat16)
            return hidden, None

        layer_ws = (ln_gain, ln_bias, w_self, b_self, w_cross_q, w_cross_kv, w_cross_o, b_cross, w_ff1, b_ff1, w_ff2, b_ff2)
        hidden, scan_out = lax.scan(block, hidden, layer_ws)
        result = project(hidden, w_out) + b_out.astype(jnp.float32) + lat_one.reshape(tokens, CHANNELS).astype(jnp.float32)
        return result.astype(jnp.bfloat16).reshape(LAT_ROWS, LAT_COLS, CHANNELS)

    return lax.map(one_sample, (latent, context))
```

```python
import functools
import math

import jax
import jax.numpy as jnp
from jax import lax
from jax.experimental import pallas as pl
from jax.experimental.pallas import tpu as pltpu
from jax.sharding import PartitionSpec as P

HEAD_DIM = 64
NUM_GROUPS = 32
CORES = 2
TILE = 256
FF_CHUNK = 512
TEXT_PAD = 128
LANES = 128
MESH = pl.DeviceIdType.MESH
F32 = jnp.float32
BF16 = jnp.bfloat16
ANY = pl.BlockSpec(memory_space=pl.ANY)
VMEM = pl.BlockSpec(memory_space=pltpu.VMEM)
NT = (((1,), (1,)), ((), ()))


def dot(a, b):
    return jnp.dot(a, b, preferred_element_type=F32)


def dot_nt(a, b):
    return lax.dot_general(a, b, NT, preferred_element_type=F32)


def layer_norm(hidden, gain, bias):
    vals = hidden.astype(F32)
    mean_val = jnp.mean(vals, axis=-1, keepdims=True)
    centered = vals - mean_val
    var_val = jnp.mean(centered * centered, axis=-1, keepdims=True)
    scaled = centered * lax.rsqrt(var_val + 1e-5)
    return (scaled * gain.astype(F32) + bias.astype(F32)).astype(BF16)


def entry_barrier(n):
    me = lax.axis_index('sp')
    sem = pltpu.get_barrier_semaphore()
    for k in range(1, n):
        pl.semaphore_signal(sem, inc=1, device_id={'sp': lax.rem(me + k, n)}, device_id_type=MESH)
    pl.semaphore_wait(sem, n - 1)


def copy_pair(k, src, dest, send_sem, recv_sem, sources, targets):
    out = []
    for i in range(2):
        if k == 0:
            out.append(pltpu.make_async_copy(sources[i], targets[i], send_sem.at[i, 0]))
        else:
            out.append(pltpu.make_async_remote_copy(
                src_ref=sources[i], dst_ref=targets[i], send_sem=send_sem.at[i, k], recv_sem=recv_sem.at[i, src],
                device_id={'sp': dest}, device_id_type=MESH))
    return out


def scatter_kernel(n, per_chip, x_ref, xs_ref, send_sem, recv_sem):
    me = lax.axis_index('sp')
    blk = x_ref.shape[1]
    part = blk // CORES
    own_rows = n * blk
    entry_barrier(n)

    def copies(k, src, dest):
        chip, core = dest // CORES, lax.rem(dest, CORES)
        return copy_pair(
            k, src, dest, send_sem, recv_sem,
            (x_ref.at[chip * per_chip + core], x_ref.at[chip * per_chip + CORES, pl.ds(pl.multiple_of(core * part, part), part)]),
            (xs_ref.at[pl.ds(pl.multiple_of(src * blk, blk), blk)],
             xs_ref.at[pl.ds(pl.multiple_of(own_rows + src * part, part), part)]))

    for k in range(n):
        for c in copies(k, me, lax.rem(me + k, n)):
            c.start()
    for k in range(n):
        src = lax.rem(me + n - k, n)
        if k == 0:
            for c in copies(k, me, me):
                c.wait()
            continue
        for c in copies(k, src, me):
            c.wait_recv()
        for c in copies(k, me, lax.rem(me + k, n)):
            c.wait_send()


def gather_kernel(n, per_chip, y_ref, out_ref, send_sem, recv_sem):
    me = lax.axis_index('sp')
    blk = out_ref.shape[1]
    part = blk // CORES
    own_rows = n * blk
    entry_barrier(n)

    def copies(k, src, dest):
        chip, core = src // CORES, lax.rem(src, CORES)
        return copy_pair(
            k, src, dest, send_sem, recv_sem,
            (y_ref.at[pl.ds(pl.multiple_of(dest * blk, blk), blk)],
             y_ref.at[pl.ds(pl.multiple_of(own_rows + dest * part, part), part)]),
            (out_ref.at[chip * per_chip + core], out_ref.at[chip * per_chip + CORES, pl.ds(pl.multiple_of(core * part, part), part)]))

    for k in range(n):
        for c in copies(k, me, lax.rem(me + k, n)):
            c.start()
    for k in range(n):
        src = lax.rem(me + n - k, n)
        if k == 0:
            for c in copies(k, me, me):
                c.wait()
            continue
        for c in copies(k, src, me):
            c.wait_recv()
        for c in copies(k, me, lax.rem(me + k, n)):
            c.wait_send()


def group_sum(row, ind):
    hi = row.astype(BF16)
    rest = row - hi.astype(F32)
    mid = rest.astype(BF16)
    low = (rest - mid.astype(F32)).astype(BF16)
    total = None
    for piece in (low, mid, hi):
        term = dot(jnp.broadcast_to(piece, (16, piece.shape[1])), ind)[0:1]
        total = term if total is None else total + term
    return total


def stats_kernel(own, group_ch, x_ref, ind_ref, st_ref):
    rows = x_ref.shape[0]
    ind = ind_ref[...]
    for row, (lo, hi) in enumerate(((0, own), (own, rows))):
        def add(i, acc):
            return acc + jnp.sum(x_ref[pl.ds(pl.multiple_of(lo + i * TILE, TILE), TILE), :].astype(F32), axis=0, keepdims=True)
        zero = jnp.zeros((1, x_ref.shape[1]), F32)
        count = float((hi - lo) * group_ch)
        mean = group_sum(lax.fori_loop(0, (hi - lo) // TILE, add, zero), ind) / count

        def sq(i, acc):
            d = x_ref[pl.ds(pl.multiple_of(lo + i * TILE, TILE), TILE), :].astype(F32) - mean
            return acc + jnp.sum(d * d, axis=0, keepdims=True)
        st_ref[2 * row:2 * row + 1, :] = mean
        st_ref[2 * row + 1:2 * row + 2, :] = group_sum(lax.fori_loop(0, (hi - lo) // TILE, sq, zero), ind)


def qkv_tile(hid, gain, bias, wqkv, r0, q_ref, k_ref, vt_ref):
    ch = hid.shape[1]
    a = layer_norm(hid, gain, bias)
    r = dot(a, wqkv[...]).astype(BF16)
    q_ref[pl.ds(r0, TILE), :] = r[:, :ch]
    k_ref[pl.ds(r0, TILE), :] = r[:, ch:2 * ch]
    vt_ref[:, pl.ds(r0, TILE)] = r[:, 2 * ch:].T


def first_kernel(own, group_ch, x_ref, st_ref, peer_ref, gng_ref, gnb_ref, win_ref, bin_ref, lng_ref, lnb_ref, wself_ref,
                 h_ref, q_ref, k_ref, vt_ref, wqkv, sem):
    rows, ch = x_ref.shape
    loads = [pltpu.make_async_copy(wself_ref.at[0, j], wqkv.at[:, pl.ds(j * ch, ch)], sem.at[j]) for j in range(3)]
    for c in loads:
        c.start()
    gain = gng_ref[...].astype(F32)
    off = gnb_ref[...].astype(F32)
    half = float((rows - own) * group_ch)
    inv_own = lax.rsqrt(st_ref[1:2, :] / float(own * group_ch) + 1e-6)
    delta = st_ref[2:3, :] - peer_ref[2:3, :]
    mean_sh = (st_ref[2:3, :] + peer_ref[2:3, :]) * 0.5
    m2 = st_ref[3:4, :] + peer_ref[3:4, :] + delta * delta * (half * 0.5)
    inv_sh = lax.rsqrt(m2 / (2.0 * half) + 1e-6)
    for c in loads:
        c.wait()

    def make(mean, inv):
        def tile(i, carry):
            r0 = pl.multiple_of(i * TILE, TILE)
            x = x_ref[pl.ds(r0, TILE), :].astype(F32)
            g = ((x - mean) * inv * gain + off).astype(BF16)
            hid = (dot(g, win_ref[...]) + bin_ref[...].astype(F32)).astype(BF16)
            h_ref[pl.ds(r0, TILE), :] = hid
            qkv_tile(hid, lng_ref[0, 0:1, :], lnb_ref[0, 0:1, :], wqkv, r0, q_ref, k_ref, vt_ref)
            return carry
        return tile
    lax.fori_loop(own // TILE, rows // TILE, make(mean_sh, inv_sh), 0)
    lax.fori_loop(0, own // TILE, make(st_ref[0:1, :], inv_own), 0)


def head_attend(kp, qp, vt, half, valid, scale):
    lane = lax.broadcasted_iota(jnp.int32, qp.shape, 1)
    qm = jnp.where((lane >= HEAD_DIM) if half else (lane < HEAD_DIM), qp, jnp.zeros_like(qp))
    s = dot_nt(kp, qm)
    if valid is not None:
        keep = lax.broadcasted_iota(jnp.int32, s.shape, 0) < valid
        s = jnp.where(keep, s, jnp.finfo(F32).min)
    top = jnp.max(s, axis=0, keepdims=True) * scale
    p = jnp.exp2(s * scale - top)
    if valid is not None:
        p = jnp.where(keep, p, 0.0)
    total = jnp.sum(p, axis=0, keepdims=True)
    return dot(vt, p.astype(BF16)) / total


def layer_kernel(layer, last, own, text_len, *refs):
    if last:
        (h_ref, q_ref, k_ref, vt_ref, kpeer_ref, vtpeer_ref, tkv_ref, lng_ref, lnb_ref, bself_ref, bcross_ref, bff1_ref, bff2_ref,
         x_ref, bout_ref, wself_ref, wcq_ref, wco_ref, wff1_ref, wff2_ref, wout_ref,
         y_ref, k_sh, vt_sh, tvt, ot, wo, wcq, wco, wff1, wff2, wout, sem) = refs
    else:
        (h_ref, q_ref, k_ref, vt_ref, kpeer_ref, vtpeer_ref, tkv_ref, lng_ref, lnb_ref, bself_ref, bcross_ref, bff1_ref, bff2_ref,
         wself_ref, wcq_ref, wco_ref, wff1_ref, wff2_ref,
         hn_ref, qn_ref, kn_ref, vtn_ref, k_sh, vt_sh, tvt, ot, wo, wcq, wco, wff1, wff2, wqkv, sem) = refs
    rows, ch = h_ref.shape
    shared = rows - own
    ff = wff2.shape[0]
    scale = HEAD_DIM ** -0.5 * math.log2(math.e)
    loads = [
        pltpu.make_async_copy(wself_ref.at[layer, 3], wo, sem.at[0]),
        pltpu.make_async_copy(wcq_ref.at[layer], wcq, sem.at[1]),
        pltpu.make_async_copy(wco_ref.at[layer], wco, sem.at[2]),
        pltpu.make_async_copy(wff1_ref.at[layer], wff1, sem.at[3]),
        pltpu.make_async_copy(wff2_ref.at[layer], wff2, sem.at[4]),
    ]
    if last:
        loads.append(pltpu.make_async_copy(wout_ref, wout, sem.at[5]))
    else:
        loads += [pltpu.make_async_copy(wself_ref.at[layer + 1, j], wqkv.at[:, pl.ds(j * ch, ch)], sem.at[5 + j]) for j in range(3)]
    for c in loads:
        c.start()
    k_sh[0:shared, :] = k_ref[own:rows, :]
    k_sh[shared:2 * shared, :] = kpeer_ref[...]
    vt_sh[:, 0:shared] = vt_ref[:, own:rows]
    vt_sh[:, shared:2 * shared] = vtpeer_ref[...]
    for s in range(2):
        tvt[s] = tkv_ref[1, s].T

    def make(slot, keys, vts):
        def tile(i, carry):
            r0 = pl.multiple_of(i * TILE, TILE)
            for pair in range(ch // LANES):
                cols = slice(pair * LANES, (pair + 1) * LANES)
                qp = q_ref[pl.ds(r0, TILE), cols]
                kp = keys[:, cols]
                for half in range(2):
                    d0 = pair * LANES + half * HEAD_DIM
                    ot[d0:d0 + HEAD_DIM, :] = head_attend(kp, qp, vts[d0:d0 + HEAD_DIM, :], half, None, scale).astype(BF16)

            @pl.when(i == first_tile[0])
            def _():
                for c in loads:
                    c.wait()
            hid = (h_ref[pl.ds(r0, TILE), :].astype(F32) + dot(ot[...].T, wo[...]) + bself_ref[layer:layer + 1, :].astype(F32)).astype(BF16)
            qc = dot(layer_norm(hid, lng_ref[layer, 1:2, :], lnb_ref[layer, 1:2, :]), wcq[...]).astype(BF16)
            for pair in range(ch // LANES):
                cols = slice(pair * LANES, (pair + 1) * LANES)
                for half in range(2):
                    d0 = pair * LANES + half * HEAD_DIM
                    ot[d0:d0 + HEAD_DIM, :] = head_attend(
                        tkv_ref[0, slot, :, cols], qc[:, cols], tvt[slot, d0:d0 + HEAD_DIM, :], half, text_len, scale).astype(BF16)
            hid = (hid.astype(F32) + dot(ot[...].T, wco[...]) + bcross_ref[layer:layer + 1, :].astype(F32)).astype(BF16)
            a = layer_norm(hid, lng_ref[layer, 2:3, :], lnb_ref[layer, 2:3, :])
            acc = None
            for c0 in range(0, ff, FF_CHUNK):
                pc, qcol = slice(c0, c0 + FF_CHUNK), slice(ff + c0, ff + c0 + FF_CHUNK)
                p = (dot(a, wff1[:, pc]) + bff1_ref[layer:layer + 1, pc].astype(F32)).astype(BF16).astype(F32)
                g = (dot(a, wff1[:, qcol]) + bff1_ref[layer:layer + 1, qcol].astype(F32)).astype(BF16).astype(F32)
                z = (p * (0.5 * g * (1.0 + lax.erf(g * math.sqrt(0.5))))).astype(BF16)
                part = dot(z, wff2[pc, :])
                acc = part if acc is None else acc + part
            hid = (hid.astype(F32) + acc + bff2_ref[layer:layer + 1, :].astype(F32)).astype(BF16)
            if last:
                y = dot(hid, wout[...]) + bout_ref[...].astype(F32) + x_ref[pl.ds(r0, TILE), :].astype(F32)
                y_ref[pl.ds(r0, TILE), :] = y.astype(BF16)
            else:
                hn_ref[pl.ds(r0, TILE), :] = hid
                qkv_tile(hid, lng_ref[layer + 1, 0:1, :], lnb_ref[layer + 1, 0:1, :], wqkv, r0, qn_ref, kn_ref, vtn_ref)
            return carry
        return tile
    first_tile = [0]
    lax.fori_loop(0, own // TILE, make(0, k_ref.at[0:own], vt_ref.at[:, 0:own]), 0)
    lax.fori_loop(own // TILE, rows // TILE, make(1, k_sh, vt_sh), 0)


def solution(mesh):
    seq_devices = mesh.shape['sp']
    tok_spec = P('dp', 'sp', None, None)
    ctx_spec = P('dp', None, None)
    replicated = P()
    shape = jax.ShapeDtypeStruct
    sem_dma = pltpu.SemaphoreType.DMA

    def local_forward(latent, context, gn_gain, gn_bias, w_in, b_in, ln_gain, ln_bias, w_self, b_self, w_cross_q, w_cross_kv, w_cross_o, b_cross, w_ff1, b_ff1, w_ff2, b_ff2, w_out, b_out):
        batch, rows, columns, ch = latent.shape
        blk = rows * columns
        group_ch = ch // NUM_GROUPS
        ff = w_ff2.shape[1]
        text_len = context.shape[1]
        per_chip = batch * CORES // seq_devices
        assert per_chip == CORES + 1
        own = seq_devices * blk
        shared = own // CORES
        toks = own + shared
        me = lax.axis_index('sp')
        base = (me // CORES) * per_chip
        core = lax.rem(me, CORES)
        peers = [(i, i ^ 1) for i in range(seq_devices)]

        ctx = jnp.stack([lax.dynamic_index_in_dim(context, base + core, 0, False), lax.dynamic_index_in_dim(context, base + CORES, 0, False)])
        ctx = jnp.pad(ctx, ((0, 0), (0, TEXT_PAD - text_len), (0, 0)))
        tkv = jnp.einsum('blc,njcd->njbld', ctx, w_cross_kv, preferred_element_type=F32).astype(BF16)

        big = pltpu.CompilerParams(vmem_limit_bytes=60 * 1024 * 1024)
        xs = pl.pallas_call(
            functools.partial(scatter_kernel, seq_devices, per_chip),
            out_shape=shape((toks, ch), BF16), in_specs=[ANY], out_specs=VMEM,
            scratch_shapes=[sem_dma((2, seq_devices)), sem_dma((2, seq_devices))],
            compiler_params=pltpu.CompilerParams(collective_id=0, has_side_effects=True),
        )(latent.reshape(batch, blk, ch))
        gid = jnp.arange(ch) // group_ch
        ind = (gid[:, None] == gid[None, :]).astype(BF16)
        st = pl.pallas_call(
            functools.partial(stats_kernel, own, group_ch),
            out_shape=shape((8, ch), F32), in_specs=[VMEM] * 2, out_specs=VMEM, compiler_params=big,
        )(xs, ind)
        st_peer = lax.ppermute(st, 'sp', peers)
        hqkv = [shape((toks, ch), BF16)] * 3 + [shape((ch, toks), BF16)]
        hid, q, k, vt = pl.pallas_call(
            functools.partial(first_kernel, own, group_ch),
            out_shape=hqkv, in_specs=[VMEM] * 9 + [ANY], out_specs=[VMEM] * 4,
            scratch_shapes=[pltpu.VMEM((ch, 3 * ch), BF16), sem_dma((3,))], compiler_params=big,
        )(xs, st, st_peer, gn_gain[None], gn_bias[None], w_in, b_in[None], ln_gain, ln_bias, w_self)
        layers = w_self.shape[0]
        for layer in range(layers):
            last = layer == layers - 1
            kp = lax.ppermute(k[own:], 'sp', peers)
            vtp = lax.ppermute(vt[:, own:], 'sp', peers)
            args = [hid, q, k, vt, kp, vtp, tkv[layer], ln_gain, ln_bias, b_self, b_cross, b_ff1, b_ff2]
            if last:
                args += [xs, b_out[None]]
            n_vmem = len(args)
            args += [w_self, w_cross_q, w_cross_o, w_ff1, w_ff2] + ([w_out] if last else [])
            scratch = [
                pltpu.VMEM((2 * shared, ch), BF16), pltpu.VMEM((ch, 2 * shared), BF16), pltpu.VMEM((2, ch, TEXT_PAD), BF16),
                pltpu.VMEM((ch, TILE), BF16), pltpu.VMEM((ch, ch), BF16), pltpu.VMEM((ch, ch), BF16), pltpu.VMEM((ch, ch), BF16),
                pltpu.VMEM((ch, 2 * ff), BF16), pltpu.VMEM((ff, ch), BF16), pltpu.VMEM((ch, ch if last else 3 * ch), BF16), sem_dma((8,))]
            res = pl.pallas_call(
                functools.partial(layer_kernel, layer, last, own, text_len),
                out_shape=shape((toks, ch), BF16) if last else hqkv,
                in_specs=[VMEM] * n_vmem + [ANY] * (len(args) - n_vmem),
                out_specs=VMEM if last else [VMEM] * 4, scratch_shapes=scratch, compiler_params=big,
            )(*args)
            if last:
                y = res
            else:
                hid, q, k, vt = res
        out = pl.pallas_call(
            functools.partial(gather_kernel, seq_devices, per_chip),
            out_shape=shape((batch, blk, ch), BF16), in_specs=[VMEM], out_specs=ANY,
            scratch_shapes=[sem_dma((2, seq_devices)), sem_dma((2, seq_devices))],
            compiler_params=pltpu.CompilerParams(collective_id=1, has_side_effects=True),
        )(y)
        return out.reshape(batch, rows, columns, ch)

    in_specs = (tok_spec, ctx_spec) + (replicated,) * 18
    return jax.shard_map(local_forward, mesh=mesh, in_specs=in_specs, out_specs=tok_spec, check_vma=False)
```

```python
import functools
import math

import jax
import jax.numpy as jnp
from jax import lax
from jax.experimental import pallas as pl
from jax.experimental.pallas import tpu as pltpu
from jax.sharding import PartitionSpec as P

HEAD_DIM = 64
NUM_GROUPS = 32
CORES = 2
TILE = 256
FF_CHUNK = 512
TEXT_PAD = 128
KEY_CHUNK = 256
LANES = 128
MESH = pl.DeviceIdType.MESH
F32 = jnp.float32
BF16 = jnp.bfloat16
ANY = pl.BlockSpec(memory_space=pl.ANY)
VMEM = pl.BlockSpec(memory_space=pltpu.VMEM)
NT = (((1,), (1,)), ((), ()))


def dot(a, b):
    return jnp.dot(a, b, preferred_element_type=F32)


def dot_nt(a, b):
    return lax.dot_general(a, b, NT, preferred_element_type=F32)


def layer_norm(hidden, gain, bias):
    vals = hidden.astype(F32)
    mean_val = jnp.mean(vals, axis=-1, keepdims=True)
    centered = vals - mean_val
    var_val = jnp.mean(centered * centered, axis=-1, keepdims=True)
    scaled = centered * lax.rsqrt(var_val + 1e-5)
    return (scaled * gain.astype(F32) + bias.astype(F32)).astype(BF16)


def entry_barrier(n):
    me = lax.axis_index('sp')
    sem = pltpu.get_barrier_semaphore()
    for k in range(1, n):
        pl.semaphore_signal(sem, inc=1, device_id={'sp': lax.rem(me + k, n)}, device_id_type=MESH)
    pl.semaphore_wait(sem, n - 1)


def copy_pair(k, src, dest, send_sem, recv_sem, sources, targets):
    out = []
    for i in range(2):
        if k == 0:
            out.append(pltpu.make_async_copy(sources[i], targets[i], send_sem.at[i, 0]))
        else:
            out.append(pltpu.make_async_remote_copy(
                src_ref=sources[i], dst_ref=targets[i], send_sem=send_sem.at[i, k], recv_sem=recv_sem.at[i, src],
                device_id={'sp': dest}, device_id_type=MESH))
    return out


def scatter_kernel(n, per_chip, x_ref, xs_ref, send_sem, recv_sem):
    me = lax.axis_index('sp')
    blk = x_ref.shape[1]
    part = blk // CORES
    own_rows = n * blk
    entry_barrier(n)

    def copies(k, src, dest):
        chip, core = dest // CORES, lax.rem(dest, CORES)
        return copy_pair(
            k, src, dest, send_sem, recv_sem,
            (x_ref.at[chip * per_chip + core], x_ref.at[chip * per_chip + CORES, pl.ds(pl.multiple_of(core * part, part), part)]),
            (xs_ref.at[pl.ds(pl.multiple_of(src * blk, blk), blk)],
             xs_ref.at[pl.ds(pl.multiple_of(own_rows + src * part, part), part)]))

    for k in range(n):
        for c in copies(k, me, lax.rem(me + k, n)):
            c.start()
    for k in range(n):
        src = lax.rem(me + n - k, n)
        if k == 0:
            for c in copies(k, me, me):
                c.wait()
            continue
        for c in copies(k, src, me):
            c.wait_recv()
        for c in copies(k, me, lax.rem(me + k, n)):
            c.wait_send()


def gather_kernel(n, per_chip, y_ref, out_ref, send_sem, recv_sem):
    me = lax.axis_index('sp')
    blk = out_ref.shape[1]
    part = blk // CORES
    own_rows = n * blk
    entry_barrier(n)

    def copies(k, src, dest):
        chip, core = src // CORES, lax.rem(src, CORES)
        return copy_pair(
            k, src, dest, send_sem, recv_sem,
            (y_ref.at[pl.ds(pl.multiple_of(dest * blk, blk), blk)],
             y_ref.at[pl.ds(pl.multiple_of(own_rows + dest * part, part), part)]),
            (out_ref.at[chip * per_chip + core], out_ref.at[chip * per_chip + CORES, pl.ds(pl.multiple_of(core * part, part), part)]))

    for k in range(n):
        for c in copies(k, me, lax.rem(me + k, n)):
            c.start()
    for k in range(n):
        src = lax.rem(me + n - k, n)
        if k == 0:
            for c in copies(k, me, me):
                c.wait()
            continue
        for c in copies(k, src, me):
            c.wait_recv()
        for c in copies(k, me, lax.rem(me + k, n)):
            c.wait_send()


def group_sum(row, ind):
    hi = row.astype(BF16)
    rest = row - hi.astype(F32)
    mid = rest.astype(BF16)
    low = (rest - mid.astype(F32)).astype(BF16)
    total = None
    for piece in (low, mid, hi):
        term = dot(jnp.broadcast_to(piece, (16, piece.shape[1])), ind)[0:1]
        total = term if total is None else total + term
    return total


def stats_kernel(own, group_ch, x_ref, ind_ref, st_ref):
    rows = x_ref.shape[0]
    ind = ind_ref[...]
    for row, (lo, hi) in enumerate(((0, own), (own, rows))):
        def add(i, acc):
            return acc + jnp.sum(x_ref[pl.ds(pl.multiple_of(lo + i * TILE, TILE), TILE), :].astype(F32), axis=0, keepdims=True)
        zero = jnp.zeros((1, x_ref.shape[1]), F32)
        count = float((hi - lo) * group_ch)
        mean = group_sum(lax.fori_loop(0, (hi - lo) // TILE, add, zero), ind) / count

        def sq(i, acc):
            d = x_ref[pl.ds(pl.multiple_of(lo + i * TILE, TILE), TILE), :].astype(F32) - mean
            return acc + jnp.sum(d * d, axis=0, keepdims=True)
        st_ref[2 * row:2 * row + 1, :] = mean
        st_ref[2 * row + 1:2 * row + 2, :] = group_sum(lax.fori_loop(0, (hi - lo) // TILE, sq, zero), ind)


def qkv_tile(hid, gain, bias, wqkv, r0, q_ref, k_ref, vt_ref):
    ch = hid.shape[1]
    a = layer_norm(hid, gain, bias)
    r = dot(a, wqkv[...]).astype(BF16)
    q_ref[pl.ds(r0, TILE), :] = r[:, :ch]
    k_ref[pl.ds(r0, TILE), :] = r[:, ch:2 * ch]
    vt_ref[:, pl.ds(r0, TILE)] = r[:, 2 * ch:].T


def first_kernel(own, group_ch, x_ref, st_ref, peer_ref, gng_ref, gnb_ref, win_ref, bin_ref, lng_ref, lnb_ref, wself_ref,
                 h_ref, q_ref, k_ref, vt_ref, wqkv, sem):
    rows, ch = x_ref.shape
    loads = [pltpu.make_async_copy(wself_ref.at[0, j], wqkv.at[:, pl.ds(j * ch, ch)], sem.at[j]) for j in range(3)]
    for c in loads:
        c.start()
    gain = gng_ref[...].astype(F32)
    off = gnb_ref[...].astype(F32)
    half = float((rows - own) * group_ch)
    inv_own = lax.rsqrt(st_ref[1:2, :] / float(own * group_ch) + 1e-6)
    delta = st_ref[2:3, :] - peer_ref[2:3, :]
    mean_sh = (st_ref[2:3, :] + peer_ref[2:3, :]) * 0.5
    m2 = st_ref[3:4, :] + peer_ref[3:4, :] + delta * delta * (half * 0.5)
    inv_sh = lax.rsqrt(m2 / (2.0 * half) + 1e-6)
    for c in loads:
        c.wait()

    def make(mean, inv):
        def tile(i, carry):
            r0 = pl.multiple_of(i * TILE, TILE)
            x = x_ref[pl.ds(r0, TILE), :].astype(F32)
            g = ((x - mean) * inv * gain + off).astype(BF16)
            hid = (dot(g, win_ref[...]) + bin_ref[...].astype(F32)).astype(BF16)
            h_ref[pl.ds(r0, TILE), :] = hid
            qkv_tile(hid, lng_ref[0, 0:1, :], lnb_ref[0, 0:1, :], wqkv, r0, q_ref, k_ref, vt_ref)
            return carry
        return tile
    lax.fori_loop(own // TILE, rows // TILE, make(mean_sh, inv_sh), 0)
    lax.fori_loop(0, own // TILE, make(st_ref[0:1, :], inv_own), 0)


def head_mask(qp, half):
    lane = lax.broadcasted_iota(jnp.int32, qp.shape, 1)
    return jnp.where((lane >= HEAD_DIM) if half else (lane < HEAD_DIM), qp, jnp.zeros_like(qp))


def self_attend(slot, r0, q_ref, k_ref, vt_ref, s0, s1, ot, scale):
    keys, ch = k_ref.shape[1:]
    pairs = ch // LANES

    def step(cur, top, d0, nxt, pair, half):
        col = pl.multiple_of(pair * LANES, LANES)
        if nxt is not None:
            qm = head_mask(q_ref[pl.ds(r0, TILE), pl.ds(col, LANES)], half)
        new_top = total = acc = None
        for c in range(0, keys, KEY_CHUNK):
            rows = slice(c, c + KEY_CHUNK)
            if nxt is not None:
                s = dot_nt(k_ref[slot, rows, pl.ds(col, LANES)], qm)
                nxt[rows, :] = s
                peak = jnp.max(s, axis=0, keepdims=True)
                new_top = peak if new_top is None else jnp.maximum(new_top, peak)
            if cur is not None:
                p = jnp.exp2(cur[rows, :] * scale - top)
                part = jnp.sum(p, axis=0, keepdims=True)
                prod = dot(vt_ref[slot, pl.ds(d0, HEAD_DIM), rows], p.astype(BF16))
                total = part if total is None else total + part
                acc = prod if acc is None else acc + prod
        if cur is not None:
            ot[pl.ds(d0, HEAD_DIM), :] = (acc / total).astype(BF16)
        return None if nxt is None else new_top * scale

    def body(pair, top):
        d0 = pl.multiple_of(pair * LANES, LANES)
        top = step(s0, top, d0, s1, pair, 1)
        return step(s1, top, pl.multiple_of(d0 + HEAD_DIM, HEAD_DIM), s0, jnp.minimum(pair + 1, pairs - 1), 0)

    lax.fori_loop(0, pairs, body, step(None, None, 0, s0, 0, 0))


def text_attend(slot, qc, tkv_ref, tvt, ot, text_len, scale):
    ch = qc.shape[1]
    used = -(-text_len // 16) * 16
    heads = ch // HEAD_DIM
    scores = []
    for h in range(heads):
        cols = slice(h // 2 * LANES, (h // 2 + 1) * LANES)
        scores.append(dot_nt(tkv_ref[0, slot, 0:used, cols], head_mask(qc[:, cols], h % 2)))
    keep = lax.broadcasted_iota(jnp.int32, scores[0].shape, 0) < text_len
    for h in range(heads):
        s = jnp.where(keep, scores[h], jnp.finfo(F32).min)
        top = jnp.max(s, axis=0, keepdims=True) * scale
        p = jnp.where(keep, jnp.exp2(s * scale - top), 0.0)
        total = jnp.sum(p, axis=0, keepdims=True)
        pb = jnp.concatenate([p.astype(BF16), jnp.zeros((TEXT_PAD - used, p.shape[1]), BF16)], axis=0)
        ot[h * HEAD_DIM:(h + 1) * HEAD_DIM, :] = (dot(tvt[slot, h * HEAD_DIM:(h + 1) * HEAD_DIM, :], pb) / total).astype(BF16)


def layer_kernel(layer, last, own, text_len, *refs):
    if last:
        (h_ref, q_ref, k_ref, vt_ref, kpeer_ref, vtpeer_ref, tkv_ref, lng_ref, lnb_ref, bself_ref, bcross_ref, bff1_ref, bff2_ref,
         x_ref, bout_ref, wself_ref, wcq_ref, wco_ref, wff1_ref, wff2_ref, wout_ref,
         y_ref, k_all, vt_all, s0, s1, tvt, ot, wo, wcq, wco, wff1, wff2, wout, sem) = refs
    else:
        (h_ref, q_ref, k_ref, vt_ref, kpeer_ref, vtpeer_ref, tkv_ref, lng_ref, lnb_ref, bself_ref, bcross_ref, bff1_ref, bff2_ref,
         wself_ref, wcq_ref, wco_ref, wff1_ref, wff2_ref,
         hn_ref, qn_ref, kn_ref, vtn_ref, k_all, vt_all, s0, s1, tvt, ot, wo, wcq, wco, wff1, wff2, wqkv, sem) = refs
    rows, ch = h_ref.shape
    shared = rows - own
    ff = wff2.shape[0]
    scale = HEAD_DIM ** -0.5 * math.log2(math.e)
    loads = [
        pltpu.make_async_copy(wself_ref.at[layer, 3], wo, sem.at[0]),
        pltpu.make_async_copy(wcq_ref.at[layer], wcq, sem.at[1]),
        pltpu.make_async_copy(wco_ref.at[layer], wco, sem.at[2]),
        pltpu.make_async_copy(wff1_ref.at[layer], wff1, sem.at[3]),
        pltpu.make_async_copy(wff2_ref.at[layer], wff2, sem.at[4]),
    ]
    if last:
        loads.append(pltpu.make_async_copy(wout_ref, wout, sem.at[5]))
    else:
        loads += [pltpu.make_async_copy(wself_ref.at[layer + 1, j], wqkv.at[:, pl.ds(j * ch, ch)], sem.at[5 + j]) for j in range(3)]
    for c in loads:
        c.start()
    k_all[0] = k_ref[0:own, :]
    vt_all[0] = vt_ref[:, 0:own]
    k_all[1, 0:shared, :] = k_ref[own:rows, :]
    k_all[1, shared:2 * shared, :] = kpeer_ref[...]
    vt_all[1, :, 0:shared] = vt_ref[:, own:rows]
    vt_all[1, :, shared:2 * shared] = vtpeer_ref[...]
    for s in range(2):
        tvt[s] = tkv_ref[1, s].T

    def tile(i, carry):
        slot = i // (own // TILE)
        r0 = pl.multiple_of(i * TILE, TILE)
        self_attend(slot, r0, q_ref, k_all, vt_all, s0, s1, ot, scale)

        @pl.when(i == 0)
        def _():
            for c in loads:
                c.wait()
        hid = (h_ref[pl.ds(r0, TILE), :].astype(F32) + dot(ot[...].T, wo[...]) + bself_ref[layer:layer + 1, :].astype(F32)).astype(BF16)
        qc = dot(layer_norm(hid, lng_ref[layer, 1:2, :], lnb_ref[layer, 1:2, :]), wcq[...]).astype(BF16)
        text_attend(slot, qc, tkv_ref, tvt, ot, text_len, scale)
        hid = (hid.astype(F32) + dot(ot[...].T, wco[...]) + bcross_ref[layer:layer + 1, :].astype(F32)).astype(BF16)
        a = layer_norm(hid, lng_ref[layer, 2:3, :], lnb_ref[layer, 2:3, :])
        acc = None
        for c0 in range(0, ff, FF_CHUNK):
            pc, qcol = slice(c0, c0 + FF_CHUNK), slice(ff + c0, ff + c0 + FF_CHUNK)
            p = (dot(a, wff1[:, pc]) + bff1_ref[layer:layer + 1, pc].astype(F32)).astype(BF16).astype(F32)
            g = (dot(a, wff1[:, qcol]) + bff1_ref[layer:layer + 1, qcol].astype(F32)).astype(BF16).astype(F32)
            z = (p * (0.5 * g * (1.0 + lax.erf(g * math.sqrt(0.5))))).astype(BF16)
            part = dot(z, wff2[pc, :])
            acc = part if acc is None else acc + part
        hid = (hid.astype(F32) + acc + bff2_ref[layer:layer + 1, :].astype(F32)).astype(BF16)
        if last:
            y = dot(hid, wout[...]) + bout_ref[...].astype(F32) + x_ref[pl.ds(r0, TILE), :].astype(F32)
            y_ref[pl.ds(r0, TILE), :] = y.astype(BF16)
        else:
            hn_ref[pl.ds(r0, TILE), :] = hid
            qkv_tile(hid, lng_ref[layer + 1, 0:1, :], lnb_ref[layer + 1, 0:1, :], wqkv, r0, qn_ref, kn_ref, vtn_ref)
        return carry
    lax.fori_loop(0, rows // TILE, tile, 0)


def solution(mesh):
    seq_devices = mesh.shape['sp']
    tok_spec = P('dp', 'sp', None, None)
    ctx_spec = P('dp', None, None)
    replicated = P()
    shape = jax.ShapeDtypeStruct
    sem_dma = pltpu.SemaphoreType.DMA

    def local_forward(latent, context, gn_gain, gn_bias, w_in, b_in, ln_gain, ln_bias, w_self, b_self, w_cross_q, w_cross_kv, w_cross_o, b_cross, w_ff1, b_ff1, w_ff2, b_ff2, w_out, b_out):
        batch, rows, columns, ch = latent.shape
        blk = rows * columns
        group_ch = ch // NUM_GROUPS
        ff = w_ff2.shape[1]
        text_len = context.shape[1]
        per_chip = batch * CORES // seq_devices
        assert per_chip == CORES + 1
        own = seq_devices * blk
        shared = own // CORES
        toks = own + shared
        me = lax.axis_index('sp')
        base = (me // CORES) * per_chip
        core = lax.rem(me, CORES)
        peers = [(i, i ^ 1) for i in range(seq_devices)]

        ctx = jnp.stack([lax.dynamic_index_in_dim(context, base + core, 0, False), lax.dynamic_index_in_dim(context, base + CORES, 0, False)])
        ctx = jnp.pad(ctx, ((0, 0), (0, TEXT_PAD - text_len), (0, 0)))
        tkv = jnp.einsum('blc,njcd->njbld', ctx, w_cross_kv, preferred_element_type=F32).astype(BF16)

        big = pltpu.CompilerParams(vmem_limit_bytes=60 * 1024 * 1024)
        xs = pl.pallas_call(
            functools.partial(scatter_kernel, seq_devices, per_chip),
            out_shape=shape((toks, ch), BF16), in_specs=[ANY], out_specs=VMEM,
            scratch_shapes=[sem_dma((2, seq_devices)), sem_dma((2, seq_devices))],
            compiler_params=pltpu.CompilerParams(collective_id=0, has_side_effects=True),
        )(latent.reshape(batch, blk, ch))
        gid = jnp.arange(ch) // group_ch
        ind = (gid[:, None] == gid[None, :]).astype(BF16)
        st = pl.pallas_call(
            functools.partial(stats_kernel, own, group_ch),
            out_shape=shape((8, ch), F32), in_specs=[VMEM] * 2, out_specs=VMEM, compiler_params=big,
        )(xs, ind)
        st_peer = lax.ppermute(st, 'sp', peers)
        hqkv = [shape((toks, ch), BF16)] * 3 + [shape((ch, toks), BF16)]
        hid, q, k, vt = pl.pallas_call(
            functools.partial(first_kernel, own, group_ch),
            out_shape=hqkv, in_specs=[VMEM] * 9 + [ANY], out_specs=[VMEM] * 4,
            scratch_shapes=[pltpu.VMEM((ch, 3 * ch), BF16), sem_dma((3,))], compiler_params=big,
        )(xs, st, st_peer, gn_gain[None], gn_bias[None], w_in, b_in[None], ln_gain, ln_bias, w_self)
        layers = w_self.shape[0]
        for layer in range(layers):
            last = layer == layers - 1
            kp = lax.ppermute(k[own:], 'sp', peers)
            vtp = lax.ppermute(vt[:, own:], 'sp', peers)
            args = [hid, q, k, vt, kp, vtp, tkv[layer], ln_gain, ln_bias, b_self, b_cross, b_ff1, b_ff2]
            if last:
                args += [xs, b_out[None]]
            n_vmem = len(args)
            args += [w_self, w_cross_q, w_cross_o, w_ff1, w_ff2] + ([w_out] if last else [])
            scratch = [
                pltpu.VMEM((2, own, ch), BF16), pltpu.VMEM((2, ch, own), BF16), pltpu.VMEM((own, TILE), F32), pltpu.VMEM((own, TILE), F32),
                pltpu.VMEM((2, ch, TEXT_PAD), BF16),
                pltpu.VMEM((ch, TILE), BF16), pltpu.VMEM((ch, ch), BF16), pltpu.VMEM((ch, ch), BF16), pltpu.VMEM((ch, ch), BF16),
                pltpu.VMEM((ch, 2 * ff), BF16), pltpu.VMEM((ff, ch), BF16), pltpu.VMEM((ch, ch if last else 3 * ch), BF16), sem_dma((8,))]
            res = pl.pallas_call(
                functools.partial(layer_kernel, layer, last, own, text_len),
                out_shape=shape((toks, ch), BF16) if last else hqkv,
                in_specs=[VMEM] * n_vmem + [ANY] * (len(args) - n_vmem),
                out_specs=VMEM if last else [VMEM] * 4, scratch_shapes=scratch, compiler_params=big,
            )(*args)
            if last:
                y = res
            else:
                hid, q, k, vt = res
        out = pl.pallas_call(
            functools.partial(gather_kernel, seq_devices, per_chip),
            out_shape=shape((batch, blk, ch), BF16), in_specs=[VMEM], out_specs=ANY,
            scratch_shapes=[sem_dma((2, seq_devices)), sem_dma((2, seq_devices))],
            compiler_params=pltpu.CompilerParams(collective_id=1, has_side_effects=True),
        )(y)
        return out.reshape(batch, rows, columns, ch)

    in_specs = (tok_spec, ctx_spec) + (replicated,) * 18
    return jax.shard_map(local_forward, mesh=mesh, in_specs=in_specs, out_specs=tok_spec, check_vma=False)
```

```python
import functools
import math

import jax
import jax.numpy as jnp
from jax import lax
from jax.experimental import pallas as pl
from jax.experimental.pallas import tpu as pltpu
from jax.sharding import PartitionSpec as P

HEAD_DIM = 64
NUM_GROUPS = 32
CORES = 2
TILE = 256
FF_CHUNK = 512
TEXT_PAD = 128
KEY_CHUNK = 256
LANES = 128
MESH = pl.DeviceIdType.MESH
F32 = jnp.float32
BF16 = jnp.bfloat16
ANY = pl.BlockSpec(memory_space=pl.ANY)
VMEM = pl.BlockSpec(memory_space=pltpu.VMEM)
NT = (((1,), (1,)), ((), ()))


def dot(a, b):
    return jnp.dot(a, b, preferred_element_type=F32)


def dot_nt(a, b):
    return lax.dot_general(a, b, NT, preferred_element_type=F32)


def layer_norm(hidden, gain, bias):
    vals = hidden.astype(F32)
    mean_val = jnp.mean(vals, axis=-1, keepdims=True)
    centered = vals - mean_val
    var_val = jnp.mean(centered * centered, axis=-1, keepdims=True)
    scaled = centered * lax.rsqrt(var_val + 1e-5)
    return (scaled * gain.astype(F32) + bias.astype(F32)).astype(BF16)


def entry_barrier(n):
    me = lax.axis_index('sp')
    sem = pltpu.get_barrier_semaphore()
    for k in range(1, n):
        pl.semaphore_signal(sem, inc=1, device_id={'sp': lax.rem(me + k, n)}, device_id_type=MESH)
    pl.semaphore_wait(sem, n - 1)


def group_sum(row, ind):
    hi = row.astype(BF16)
    rest = row - hi.astype(F32)
    mid = rest.astype(BF16)
    low = (rest - mid.astype(F32)).astype(BF16)
    total = None
    for piece in (low, mid, hi):
        term = dot(jnp.broadcast_to(piece, (16, piece.shape[1])), ind)[0:1]
        total = term if total is None else total + term
    return total


def same_group(ch, group_ch):
    def gid(axis):
        pos = lax.broadcasted_iota(jnp.int32, (ch, ch), axis).astype(F32)
        return jnp.floor((pos + 0.5) * (1.0 / group_ch))
    return jnp.where(gid(0) == gid(1), 1.0, 0.0).astype(BF16)


def column_stats(x_ref, lo, hi, count, ind):
    steps = (hi - lo) // TILE
    zero = jnp.zeros((1, x_ref.shape[1]), F32)

    def rows(i):
        return x_ref[pl.ds(pl.multiple_of(lo + i * TILE, TILE), TILE), :].astype(F32)

    mean = group_sum(lax.fori_loop(0, steps, lambda i, acc: acc + jnp.sum(rows(i), axis=0, keepdims=True), zero), ind) / count

    def sq(i, acc):
        d = rows(i) - mean
        return acc + jnp.sum(d * d, axis=0, keepdims=True)
    return mean, group_sum(lax.fori_loop(0, steps, sq, zero), ind)


def qkv_tile(hid, gain, bias, wqkv, slot, r0, k0, q_ref, k_ref, vt_ref):
    ch = hid.shape[1]
    a = layer_norm(hid, gain, bias)
    r = dot(a, wqkv[...]).astype(BF16)
    q_ref[pl.ds(r0, TILE), :] = r[:, :ch]
    k_ref[slot, pl.ds(k0, TILE), :] = r[:, ch:2 * ch]
    vt_ref[slot, :, pl.ds(k0, TILE)] = r[:, 2 * ch:].T


def head_mask(qp, half):
    lane = lax.broadcasted_iota(jnp.int32, qp.shape, 1)
    return jnp.where((lane >= HEAD_DIM) if half else (lane < HEAD_DIM), qp, jnp.zeros_like(qp))


def self_attend(slot, r0, q_ref, k_ref, vt_ref, s0, s1, ot, scale):
    keys, ch = k_ref.shape[1:]
    pairs = ch // LANES

    def step(cur, top, d0, nxt, pair, half):
        col = pl.multiple_of(pair * LANES, LANES)
        if nxt is not None:
            qm = head_mask(q_ref[pl.ds(r0, TILE), pl.ds(col, LANES)], half)
        new_top = total = acc = None
        for c in range(0, keys, KEY_CHUNK):
            rows = slice(c, c + KEY_CHUNK)
            if nxt is not None:
                s = dot_nt(k_ref[slot, rows, pl.ds(col, LANES)], qm)
                nxt[rows, :] = s
                peak = jnp.max(s, axis=0, keepdims=True)
                new_top = peak if new_top is None else jnp.maximum(new_top, peak)
            if cur is not None:
                p = jnp.exp2(cur[rows, :] * scale - top)
                part = jnp.sum(p, axis=0, keepdims=True)
                prod = dot(vt_ref[slot, pl.ds(d0, HEAD_DIM), rows], p.astype(BF16))
                total = part if total is None else total + part
                acc = prod if acc is None else acc + prod
        if cur is not None:
            ot[pl.ds(d0, HEAD_DIM), :] = (acc / total).astype(BF16)
        return None if nxt is None else new_top * scale

    def body(pair, top):
        d0 = pl.multiple_of(pair * LANES, LANES)
        top = step(s0, top, d0, s1, pair, 1)
        return step(s1, top, pl.multiple_of(d0 + HEAD_DIM, HEAD_DIM), s0, lax.rem(pair + 1, pairs), 0)

    lax.fori_loop(0, pairs, body, step(None, None, 0, s0, 0, 0))


def text_attend(layer, slot, qc, tk, tvt, ot, text_len, scale):
    ch = qc.shape[1]
    used = -(-text_len // 16) * 16
    heads = ch // HEAD_DIM
    scores = []
    for h in range(heads):
        cols = slice(h // 2 * LANES, (h // 2 + 1) * LANES)
        scores.append(dot_nt(tk[layer, slot, 0:used, cols], head_mask(qc[:, cols], h % 2)))
    keep = lax.broadcasted_iota(jnp.int32, scores[0].shape, 0) < text_len
    for h in range(heads):
        s = jnp.where(keep, scores[h], jnp.finfo(F32).min)
        top = jnp.max(s, axis=0, keepdims=True) * scale
        p = jnp.where(keep, jnp.exp2(s * scale - top), 0.0)
        total = jnp.sum(p, axis=0, keepdims=True)
        pb = jnp.concatenate([p.astype(BF16), jnp.zeros((TEXT_PAD - used, p.shape[1]), BF16)], axis=0)
        ot[h * HEAD_DIM:(h + 1) * HEAD_DIM, :] = (dot(tvt[layer, slot, h * HEAD_DIM:(h + 1) * HEAD_DIM, :], pb) / total).astype(BF16)


def whole_kernel(n, per_chip, group_ch,
                 gng_ref, gnb_ref, bin_ref, lng_ref, lnb_ref, bself_ref, bcross_ref, bff1_ref, bff2_ref, bout_ref,
                 x_ref, ctx_ref, win_ref, wself_ref, wcq_ref, wxkv_ref, wco_ref, wff1_ref, wff2_ref, wout_ref,
                 out_ref,
                 xs, hs, qs, k0, k1, vt0, vt1, s0, s1, ot, tk, tvt, vtmp, ctx, wx, win, wout, wo, wcq, wco, wff1, wff2, wqkv,
                 st_mine, st_peer, in_send, in_recv, out_send, out_recv, local_sem, st_sem, kv_send, kv_recv, w_sem, c_sem, x_sem):
    me = lax.axis_index('sp')
    chip, core = me // CORES, lax.rem(me, CORES)
    peer = chip * CORES + (CORES - 1 - core)
    blk, ch = x_ref.shape[1:]
    part = blk // CORES
    own = n * blk
    rows = xs.shape[0]
    shared = rows - own
    ff = wff2.shape[0]
    text_len = ctx_ref.shape[1]
    own_tiles, sh_tiles = own // TILE, shared // TILE
    scale = HEAD_DIM ** -0.5 * math.log2(math.e)
    ks, vts = (k0, k1), (vt0, vt1)
    layers = wself_ref.shape[0]

    ctx_loads = [pltpu.make_async_copy(ctx_ref.at[chip * per_chip + core], ctx.at[0], c_sem.at[0]),
                 pltpu.make_async_copy(ctx_ref.at[chip * per_chip + CORES], ctx.at[1], c_sem.at[1])]

    def text_loads(layer):
        return [pltpu.make_async_copy(wxkv_ref.at[layer, j], wx.at[j], x_sem.at[j]) for j in range(2)]

    def qkv_loads(layer):
        return [pltpu.make_async_copy(wself_ref.at[layer, j], wqkv.at[:, pl.ds(j * ch, ch)], w_sem.at[j]) for j in range(3)]

    def layer_loads(layer):
        pairs = ((wself_ref.at[layer, 3], wo), (wcq_ref.at[layer], wcq), (wco_ref.at[layer], wco), (wff1_ref.at[layer], wff1), (wff2_ref.at[layer], wff2))
        return [pltpu.make_async_copy(src, dst, w_sem.at[3 + j]) for j, (src, dst) in enumerate(pairs)]

    edge_loads = [pltpu.make_async_copy(win_ref, win, w_sem.at[8]), pltpu.make_async_copy(wout_ref, wout, w_sem.at[9])]

    def begin(copies):
        for c in copies:
            c.start()

    def finish(copies):
        for c in copies:
            c.wait()

    def in_copy(i, src, dest):
        to_chip, to_core = dest // CORES, lax.rem(dest, CORES)
        source = (x_ref.at[to_chip * per_chip + to_core],
                  x_ref.at[to_chip * per_chip + CORES, pl.ds(pl.multiple_of(to_core * part, part), part)])[i]
        target = (xs.at[pl.ds(pl.multiple_of(src * blk, blk), blk)],
                  xs.at[pl.ds(pl.multiple_of(own + src * part, part), part)])[i]
        return source, target

    def in_remote(i, src, dest):
        source, target = in_copy(i, src, dest)
        return pltpu.make_async_remote_copy(
            src_ref=source, dst_ref=target, send_sem=in_send.at[i, dest], recv_sem=in_recv.at[i, src],
            device_id={'sp': dest}, device_id_type=MESH)

    def out_copy(i, src, dest):
        from_chip, from_core = src // CORES, lax.rem(src, CORES)
        source = (xs.at[pl.ds(pl.multiple_of(dest * blk, blk), blk)],
                  xs.at[pl.ds(pl.multiple_of(own + dest * part, part), part)])[i]
        target = (out_ref.at[from_chip * per_chip + from_core],
                  out_ref.at[from_chip * per_chip + CORES, pl.ds(pl.multiple_of(from_core * part, part), part)])[i]
        return source, target

    def out_remote(i, src, dest):
        source, target = out_copy(i, src, dest)
        return pltpu.make_async_remote_copy(
            src_ref=source, dst_ref=target, send_sem=out_send.at[i, dest], recv_sem=out_recv.at[i, src],
            device_id={'sp': dest}, device_id_type=MESH)

    def out_local(i):
        source, target = out_copy(i, me, me)
        return pltpu.make_async_copy(source, target, local_sem.at[2 + i])

    def send_out(i, dest):
        @pl.when(dest != me)
        def _():
            out_remote(i, me, dest).start()

        @pl.when(dest == me)
        def _():
            out_local(i).start()

    def kv_copies(layer):
        k, vt = ks[layer], vts[layer]
        args = ((k.at[1, pl.ds(0, shared)], k.at[1, pl.ds(shared, shared)]),
                (vt.at[1, :, pl.ds(0, shared)], vt.at[1, :, pl.ds(shared, shared)]))
        return [pltpu.make_async_remote_copy(
            src_ref=a, dst_ref=b, send_sem=kv_send.at[layer, j], recv_sem=kv_recv.at[layer, j],
            device_id={'sp': peer}, device_id_type=MESH) for j, (a, b) in enumerate(args)]

    begin(ctx_loads)
    begin(text_loads(0))
    locals_in = [pltpu.make_async_copy(*in_copy(i, me, me), local_sem.at[i]) for i in range(2)]
    begin(locals_in)
    entry_barrier(n)
    for i in (1, 0):
        for k in range(1, n):
            in_remote(i, me, lax.rem(me + k, n)).start()
    begin(edge_loads)
    begin(qkv_loads(0))

    tk[...] = jnp.zeros_like(tk)
    vtmp[...] = jnp.zeros_like(vtmp)
    finish(ctx_loads)
    for layer in range(layers):
        finish(text_loads(layer))
        for s in range(2):
            tk[layer, s, 0:text_len, :] = dot(ctx[s], wx[0]).astype(BF16)
            vtmp[0:text_len, :] = dot(ctx[s], wx[1]).astype(BF16)
            tvt[layer, s] = vtmp[...].T
        if layer + 1 < layers:
            begin(text_loads(layer + 1))
    begin(layer_loads(0))
    ind = same_group(ch, group_ch)

    locals_in[1].wait()
    for k in range(1, n):
        in_remote(1, lax.rem(me + k, n), me).wait_recv()
    half = float(shared * group_ch)
    mean, m2 = column_stats(xs, own, rows, half, ind)
    st_mine[...] = jnp.zeros_like(st_mine)
    st_mine[0:1, :] = mean
    st_mine[1:2, :] = m2
    st_copy = pltpu.make_async_remote_copy(
        src_ref=st_mine, dst_ref=st_peer, send_sem=st_sem.at[0], recv_sem=st_sem.at[1], device_id={'sp': peer}, device_id_type=MESH)
    st_copy.start()
    finish(edge_loads)
    finish(qkv_loads(0))
    st_copy.wait()
    delta = mean - st_peer[0:1, :]
    mean_sh = (mean + st_peer[0:1, :]) * 0.5
    m2 = m2 + st_peer[1:2, :] + delta * delta * (half * 0.5)
    inv_sh = lax.rsqrt(m2 / (2.0 * half) + 1e-6)
    gain = gng_ref[...].astype(F32)
    off = gnb_ref[...].astype(F32)

    def enter(slot, mean, inv):
        def tile(i, carry):
            r0 = pl.multiple_of(slot * own + i * TILE, TILE)
            x = xs[pl.ds(r0, TILE), :].astype(F32)
            g = ((x - mean) * inv * gain + off).astype(BF16)
            hid = (dot(g, win[...]) + bin_ref[...].astype(F32)).astype(BF16)
            hs[pl.ds(r0, TILE), :] = hid
            qkv_tile(hid, lng_ref[0, 0:1, :], lnb_ref[0, 0:1, :], wqkv, slot, r0, pl.multiple_of(i * TILE, TILE), qs, k0, vt0)
            return carry
        return tile
    lax.fori_loop(0, sh_tiles, enter(1, mean_sh, inv_sh), 0)
    begin(kv_copies(0))

    locals_in[0].wait()
    for k in range(1, n):
        in_remote(0, lax.rem(me + k, n), me).wait_recv()
    count = float(own * group_ch)
    mean, m2 = column_stats(xs, 0, own, count, ind)
    lax.fori_loop(0, own_tiles, enter(0, mean, lax.rsqrt(m2 / count + 1e-6)), 0)

    for layer in range(layers):
        last = layer == layers - 1
        k_all, vt_all = ks[layer], vts[layer]
        loads = layer_loads(layer)
        if layer:
            begin(loads)
        if not last:
            begin(qkv_loads(layer + 1))
        for c in kv_copies(layer):
            c.wait_recv()

        def tile(it, carry):
            f = (it + own_tiles - sh_tiles) // own_tiles
            slot = 1 - f
            idx = f * lax.rem(chip + 1 + it + own_tiles - sh_tiles, own_tiles) + slot * (own_tiles + it)
            r0 = pl.multiple_of(idx * TILE, TILE)
            k0r = pl.multiple_of(idx * TILE - slot * own, TILE)
            self_attend(slot, r0, qs, k_all, vt_all, s0, s1, ot, scale)

            @pl.when(it == 0)
            def _():
                finish(loads)
                if not last:
                    finish(qkv_loads(layer + 1))
            hid = (hs[pl.ds(r0, TILE), :].astype(F32) + dot(ot[...].T, wo[...]) + bself_ref[layer:layer + 1, :].astype(F32)).astype(BF16)
            qc = dot(layer_norm(hid, lng_ref[1, layer:layer + 1, :], lnb_ref[1, layer:layer + 1, :]), wcq[...]).astype(BF16)
            text_attend(layer, slot, qc, tk, tvt, ot, text_len, scale)
            hid = (hid.astype(F32) + dot(ot[...].T, wco[...]) + bcross_ref[layer:layer + 1, :].astype(F32)).astype(BF16)
            a = layer_norm(hid, lng_ref[2, layer:layer + 1, :], lnb_ref[2, layer:layer + 1, :])
            acc = None
            for c0 in range(0, ff, FF_CHUNK):
                pc, qcol = slice(c0, c0 + FF_CHUNK), slice(ff + c0, ff + c0 + FF_CHUNK)
                p = (dot(a, wff1[:, pc]) + bff1_ref[layer:layer + 1, pc].astype(F32)).astype(BF16).astype(F32)
                g = (dot(a, wff1[:, qcol]) + bff1_ref[layer:layer + 1, qcol].astype(F32)).astype(BF16).astype(F32)
                z = (p * (0.5 * g * (1.0 + lax.erf(g * math.sqrt(0.5))))).astype(BF16)
                prod = dot(z, wff2[pc, :])
                acc = prod if acc is None else acc + prod
            hid = (hid.astype(F32) + acc + bff2_ref[layer:layer + 1, :].astype(F32)).astype(BF16)
            if last:
                y = dot(hid, wout[...]) + bout_ref[...].astype(F32) + xs[pl.ds(r0, TILE), :].astype(F32)
                xs[pl.ds(r0, TILE), :] = y.astype(BF16)

                @pl.when(slot == 0)
                def _():
                    for j in range(TILE // blk):
                        send_out(0, idx * (TILE // blk) + j)

                @pl.when(slot == 1)
                def _():
                    for j in range(TILE // part):
                        send_out(1, (idx - own_tiles) * (TILE // part) + j)
            else:
                hs[pl.ds(r0, TILE), :] = hid
                qkv_tile(hid, lng_ref[0, layer + 1:layer + 2, :], lnb_ref[0, layer + 1:layer + 2, :], wqkv, slot, r0, k0r, qs,
                         ks[layer + 1], vts[layer + 1])

                @pl.when(it == sh_tiles - 1)
                def _():
                    begin(kv_copies(layer + 1))
            return carry
        lax.fori_loop(0, own_tiles + sh_tiles, tile, 0)

    for layer in range(layers):
        for c in kv_copies(layer):
            c.wait_send()
    for i in range(2):
        out_local(i).wait()
        for k in range(1, n):
            other = lax.rem(me + k, n)
            in_remote(i, me, other).wait_send()
            out_remote(i, me, other).wait_send()
            out_remote(i, other, me).wait_recv()


def solution(mesh):
    n = mesh.shape['sp']
    tok_spec = P('dp', 'sp', None, None)
    ctx_spec = P('dp', None, None)
    replicated = P()
    dma = pltpu.SemaphoreType.DMA

    def local_forward(latent, context, gn_gain, gn_bias, w_in, b_in, ln_gain, ln_bias, w_self, b_self, w_cross_q, w_cross_kv, w_cross_o, b_cross, w_ff1, b_ff1, w_ff2, b_ff2, w_out, b_out):
        batch, rows, columns, ch = latent.shape
        blk = rows * columns
        ff = w_ff2.shape[1]
        layers, text_len, text_dim = w_self.shape[0], context.shape[1], context.shape[2]
        per_chip = batch * CORES // n
        assert per_chip == CORES + 1 and layers == 2
        own = n * blk
        toks = own + own // CORES

        def vm(*dims, dtype=BF16):
            return pltpu.VMEM(dims, dtype)

        scratch = [
            vm(toks, ch), vm(toks, ch), vm(toks, ch), vm(2, own, ch), vm(2, own, ch), vm(2, ch, own), vm(2, ch, own),
            vm(own, TILE, dtype=F32), vm(own, TILE, dtype=F32), vm(ch, TILE),
            vm(layers, 2, TEXT_PAD, ch), vm(layers, 2, ch, TEXT_PAD), vm(TEXT_PAD, ch), vm(2, text_len, text_dim), vm(2, text_dim, ch),
            vm(ch, ch), vm(ch, ch), vm(ch, ch), vm(ch, ch), vm(ch, ch), vm(ch, 2 * ff), vm(ff, ch), vm(ch, 3 * ch),
            vm(8, ch, dtype=F32), vm(8, ch, dtype=F32),
            dma((2, n)), dma((2, n)), dma((2, n)), dma((2, n)), dma((4,)), dma((2,)), dma((layers, 2)), dma((layers, 2)), dma((10,)), dma((2,)), dma((2,))]
        small = [gn_gain[None], gn_bias[None], b_in[None], ln_gain.transpose(1, 0, 2), ln_bias.transpose(1, 0, 2), b_self, b_cross, b_ff1, b_ff2, b_out[None]]
        big = [latent.reshape(batch, blk, ch), context, w_in, w_self, w_cross_q, w_cross_kv, w_cross_o, w_ff1, w_ff2, w_out]
        out = pl.pallas_call(
            functools.partial(whole_kernel, n, per_chip, ch // NUM_GROUPS),
            out_shape=jax.ShapeDtypeStruct((batch, blk, ch), BF16),
            in_specs=[VMEM] * len(small) + [ANY] * len(big), out_specs=ANY, scratch_shapes=scratch,
            compiler_params=pltpu.CompilerParams(collective_id=0, has_side_effects=True, vmem_limit_bytes=62 * 1024 * 1024),
        )(*small, *big)
        return out.reshape(batch, rows, columns, ch)

    in_specs = (tok_spec, ctx_spec) + (replicated,) * 18
    return jax.shard_map(local_forward, mesh=mesh, in_specs=in_specs, out_specs=tok_spec, check_vma=False)
```

```python
import functools
import math

import jax
import jax.numpy as jnp
from jax import lax
from jax.experimental import pallas as pl
from jax.experimental.pallas import tpu as pltpu
from jax.sharding import PartitionSpec as P

HEAD_DIM = 64
NUM_GROUPS = 32
CORES = 2
TILE = 256
FF_CHUNK = 512
TEXT_PAD = 128
KEY_CHUNK = 256
LANES = 128
MESH = pl.DeviceIdType.MESH
F32 = jnp.float32
BF16 = jnp.bfloat16
ANY = pl.BlockSpec(memory_space=pl.ANY)
VMEM = pl.BlockSpec(memory_space=pltpu.VMEM)
NT = (((1,), (1,)), ((), ()))


def dot(a, b):
    return jnp.dot(a, b, preferred_element_type=F32)


def dot_nt(a, b):
    return lax.dot_general(a, b, NT, preferred_element_type=F32)


def layer_norm(hidden, gain, bias):
    vals = hidden.astype(F32)
    mean_val = jnp.mean(vals, axis=-1, keepdims=True)
    centered = vals - mean_val
    var_val = jnp.mean(centered * centered, axis=-1, keepdims=True)
    scaled = centered * lax.rsqrt(var_val + 1e-5)
    return (scaled * gain.astype(F32) + bias.astype(F32)).astype(BF16)


def entry_barrier(n):
    me = lax.axis_index('sp')
    sem = pltpu.get_barrier_semaphore()
    for k in range(1, n):
        pl.semaphore_signal(sem, inc=1, device_id={'sp': lax.rem(me + k, n)}, device_id_type=MESH)
    pl.semaphore_wait(sem, n - 1)


def group_sum(row, ind):
    hi = row.astype(BF16)
    rest = row - hi.astype(F32)
    mid = rest.astype(BF16)
    low = (rest - mid.astype(F32)).astype(BF16)
    total = None
    for piece in (low, mid, hi):
        term = dot(jnp.broadcast_to(piece, (16, piece.shape[1])), ind)[0:1]
        total = term if total is None else total + term
    return total


def same_group(ch, group_ch):
    def gid(axis):
        pos = lax.broadcasted_iota(jnp.int32, (ch, ch), axis).astype(F32)
        return jnp.floor((pos + 0.5) * (1.0 / group_ch))
    return jnp.where(gid(0) == gid(1), 1.0, 0.0).astype(BF16)


def column_stats(x_ref, lo, hi, count, ind):
    steps = (hi - lo) // TILE
    zero = jnp.zeros((1, x_ref.shape[1]), F32)

    def rows(i):
        return x_ref[pl.ds(pl.multiple_of(lo + i * TILE, TILE), TILE), :].astype(F32)

    mean = group_sum(lax.fori_loop(0, steps, lambda i, acc: acc + jnp.sum(rows(i), axis=0, keepdims=True), zero), ind) / count

    def sq(i, acc):
        d = rows(i) - mean
        return acc + jnp.sum(d * d, axis=0, keepdims=True)
    return mean, group_sum(lax.fori_loop(0, steps, sq, zero), ind)


def qkv_tile(hid, gain, bias, wqkv, slot, r0, k0, q_ref, k_ref, vt_ref):
    ch = hid.shape[1]
    a = layer_norm(hid, gain, bias)
    r = dot(a, wqkv[...]).astype(BF16)
    q_ref[pl.ds(r0, TILE), :] = r[:, :ch]
    k_ref[slot, pl.ds(k0, TILE), :] = r[:, ch:2 * ch]
    vt_ref[slot, :, pl.ds(k0, TILE)] = r[:, 2 * ch:].T


def head_mask(qp, half):
    lane = lax.broadcasted_iota(jnp.int32, qp.shape, 1)
    return jnp.where((lane >= HEAD_DIM) if half else (lane < HEAD_DIM), qp, jnp.zeros_like(qp))


def self_attend(slot, r0, q_ref, k_ref, vt_ref, s0, s1, ot, scale):
    keys, ch = k_ref.shape[1:]
    pairs = ch // LANES

    def step(cur, top, d0, nxt, pair, half):
        col = pl.multiple_of(pair * LANES, LANES)
        if nxt is not None:
            qm = head_mask(q_ref[pl.ds(r0, TILE), pl.ds(col, LANES)], half)
        new_top = total = acc = None
        for c in range(0, keys, KEY_CHUNK):
            rows = slice(c, c + KEY_CHUNK)
            if nxt is not None:
                s = dot_nt(k_ref[slot, rows, pl.ds(col, LANES)], qm)
                nxt[rows, :] = s
                peak = jnp.max(s, axis=0, keepdims=True)
                new_top = peak if new_top is None else jnp.maximum(new_top, peak)
            if cur is not None:
                p = jnp.exp2(cur[rows, :] * scale - top)
                part = jnp.sum(p, axis=0, keepdims=True)
                prod = dot(vt_ref[slot, pl.ds(d0, HEAD_DIM), rows], p.astype(BF16))
                total = part if total is None else total + part
                acc = prod if acc is None else acc + prod
        if cur is not None:
            ot[pl.ds(d0, HEAD_DIM), :] = (acc / total).astype(BF16)
        return None if nxt is None else new_top * scale

    def body(pair, top):
        d0 = pl.multiple_of(pair * LANES, LANES)
        top = step(s0, top, d0, s1, pair, 1)
        return step(s1, top, pl.multiple_of(d0 + HEAD_DIM, HEAD_DIM), s0, lax.rem(pair + 1, pairs), 0)

    lax.fori_loop(0, pairs, body, step(None, None, 0, s0, 0, 0))


def text_attend(layer, slot, qc, tk, tvt, ot, text_len, scale):
    ch = qc.shape[1]
    used = -(-text_len // 16) * 16
    heads = ch // HEAD_DIM
    scores = []
    for h in range(heads):
        cols = slice(h // 2 * LANES, (h // 2 + 1) * LANES)
        scores.append(dot_nt(tk[layer, slot, 0:used, cols], head_mask(qc[:, cols], h % 2)))
    keep = lax.broadcasted_iota(jnp.int32, scores[0].shape, 0) < text_len
    for h in range(heads):
        s = jnp.where(keep, scores[h], jnp.finfo(F32).min)
        top = jnp.max(s, axis=0, keepdims=True) * scale
        p = jnp.where(keep, jnp.exp2(s * scale - top), 0.0)
        total = jnp.sum(p, axis=0, keepdims=True)
        pb = jnp.concatenate([p.astype(BF16), jnp.zeros((TEXT_PAD - used, p.shape[1]), BF16)], axis=0)
        ot[h * HEAD_DIM:(h + 1) * HEAD_DIM, :] = (dot(tvt[layer, slot, h * HEAD_DIM:(h + 1) * HEAD_DIM, :], pb) / total).astype(BF16)


def whole_kernel(n, per_chip, group_ch,
                 gng_ref, gnb_ref, bin_ref, lng_ref, lnb_ref, bself_ref, bcross_ref, bff1_ref, bff2_ref, bout_ref,
                 x_ref, ctx_ref, win_ref, wself_ref, wcq_ref, wxkv_ref, wco_ref, wff1_ref, wff2_ref, wout_ref,
                 out_ref,
                 xs, hs, qs, k0, k1, vt0, vt1, s0, s1, ot, tk, tvt, vtmp, ctx, wx, win, wout, wo, wcq, wco, wff1, wff2, wqkv0, wqkv1,
                 st_mine, st_peer, in_send, in_recv, out_send, out_recv, local_sem, st_sem, kv_send, kv_recv, w_sem, c_sem, x_sem):
    me = lax.axis_index('sp')
    chip, core = me // CORES, lax.rem(me, CORES)
    peer = chip * CORES + (CORES - 1 - core)
    blk, ch = x_ref.shape[1:]
    part = blk // CORES
    own = n * blk
    rows = xs.shape[0]
    shared = rows - own
    ff = wff2.shape[0]
    text_len = ctx_ref.shape[1]
    own_tiles, sh_tiles = own // TILE, shared // TILE
    scale = HEAD_DIM ** -0.5 * math.log2(math.e)
    ks, vts, wqkvs = (k0, k1), (vt0, vt1), (wqkv0, wqkv1)
    layers = wself_ref.shape[0]

    ctx_loads = [pltpu.make_async_copy(ctx_ref.at[chip * per_chip + core], ctx.at[0], c_sem.at[0]),
                 pltpu.make_async_copy(ctx_ref.at[chip * per_chip + CORES], ctx.at[1], c_sem.at[1])]

    def text_loads(layer):
        return [pltpu.make_async_copy(wxkv_ref.at[layer, j], wx.at[j], x_sem.at[j]) for j in range(2)]

    def qkv_loads(layer):
        return [pltpu.make_async_copy(wself_ref.at[layer, j], wqkvs[layer].at[:, pl.ds(j * ch, ch)], w_sem.at[10 * layer + j]) for j in range(3)]

    def layer_loads(layer):
        pairs = ((wself_ref.at[layer, 3], wo), (wcq_ref.at[layer], wcq), (wco_ref.at[layer], wco), (wff1_ref.at[layer], wff1), (wff2_ref.at[layer], wff2))
        return [pltpu.make_async_copy(src, dst, w_sem.at[3 + j]) for j, (src, dst) in enumerate(pairs)]

    edge_loads = [pltpu.make_async_copy(win_ref, win, w_sem.at[8]), pltpu.make_async_copy(wout_ref, wout, w_sem.at[9])]

    def begin(copies):
        for c in copies:
            c.start()

    def finish(copies):
        for c in copies:
            c.wait()

    def in_copy(i, src, dest):
        to_chip, to_core = dest // CORES, lax.rem(dest, CORES)
        source = (x_ref.at[to_chip * per_chip + to_core],
                  x_ref.at[to_chip * per_chip + CORES, pl.ds(pl.multiple_of(to_core * part, part), part)])[i]
        target = (xs.at[pl.ds(pl.multiple_of(src * blk, blk), blk)],
                  xs.at[pl.ds(pl.multiple_of(own + src * part, part), part)])[i]
        return source, target

    def in_remote(i, src, dest):
        source, target = in_copy(i, src, dest)
        return pltpu.make_async_remote_copy(
            src_ref=source, dst_ref=target, send_sem=in_send.at[i, dest], recv_sem=in_recv.at[i, src],
            device_id={'sp': dest}, device_id_type=MESH)

    def out_copy(i, src, dest):
        from_chip, from_core = src // CORES, lax.rem(src, CORES)
        source = (xs.at[pl.ds(pl.multiple_of(dest * blk, blk), blk)],
                  xs.at[pl.ds(pl.multiple_of(own + dest * part, part), part)])[i]
        target = (out_ref.at[from_chip * per_chip + from_core],
                  out_ref.at[from_chip * per_chip + CORES, pl.ds(pl.multiple_of(from_core * part, part), part)])[i]
        return source, target

    def out_remote(i, src, dest):
        source, target = out_copy(i, src, dest)
        return pltpu.make_async_remote_copy(
            src_ref=source, dst_ref=target, send_sem=out_send.at[i, dest], recv_sem=out_recv.at[i, src],
            device_id={'sp': dest}, device_id_type=MESH)

    def out_local(i):
        source, target = out_copy(i, me, me)
        return pltpu.make_async_copy(source, target, local_sem.at[2 + i])

    def send_out(i, dest):
        @pl.when(dest != me)
        def _():
            out_remote(i, me, dest).start()

        @pl.when(dest == me)
        def _():
            out_local(i).start()

    def kv_copies(layer):
        k, vt = ks[layer], vts[layer]
        args = ((k.at[1, pl.ds(0, shared)], k.at[1, pl.ds(shared, shared)]),
                (vt.at[1, :, pl.ds(0, shared)], vt.at[1, :, pl.ds(shared, shared)]))
        return [pltpu.make_async_remote_copy(
            src_ref=a, dst_ref=b, send_sem=kv_send.at[layer, j], recv_sem=kv_recv.at[layer, j],
            device_id={'sp': peer}, device_id_type=MESH) for j, (a, b) in enumerate(args)]

    begin(ctx_loads)
    begin(text_loads(0))
    locals_in = [pltpu.make_async_copy(*in_copy(i, me, me), local_sem.at[i]) for i in range(2)]
    begin(locals_in)
    entry_barrier(n)
    for i in (1, 0):
        for k in range(1, n):
            in_remote(i, me, lax.rem(me + k, n)).start()
    begin(edge_loads)
    begin(qkv_loads(0))

    tk[...] = jnp.zeros_like(tk)
    vtmp[...] = jnp.zeros_like(vtmp)
    finish(ctx_loads)
    for layer in range(layers):
        finish(text_loads(layer))
        for s in range(2):
            tk[layer, s, 0:text_len, :] = dot(ctx[s], wx[0]).astype(BF16)
            vtmp[0:text_len, :] = dot(ctx[s], wx[1]).astype(BF16)
            tvt[layer, s] = vtmp[...].T
        if layer + 1 < layers:
            begin(text_loads(layer + 1))
    begin(layer_loads(0))
    begin(qkv_loads(1))
    ind = same_group(ch, group_ch)

    locals_in[1].wait()
    for k in range(1, n):
        in_remote(1, lax.rem(me + k, n), me).wait_recv()
    half = float(shared * group_ch)
    mean, m2 = column_stats(xs, own, rows, half, ind)
    st_mine[...] = jnp.zeros_like(st_mine)
    st_mine[0:1, :] = mean
    st_mine[1:2, :] = m2
    st_copy = pltpu.make_async_remote_copy(
        src_ref=st_mine, dst_ref=st_peer, send_sem=st_sem.at[0], recv_sem=st_sem.at[1], device_id={'sp': peer}, device_id_type=MESH)
    st_copy.start()
    finish(edge_loads)
    finish(qkv_loads(0))
    st_copy.wait()
    delta = mean - st_peer[0:1, :]
    mean_sh = (mean + st_peer[0:1, :]) * 0.5
    m2 = m2 + st_peer[1:2, :] + delta * delta * (half * 0.5)
    inv_sh = lax.rsqrt(m2 / (2.0 * half) + 1e-6)
    gain = gng_ref[...].astype(F32)[None, :]
    off = gnb_ref[...].astype(F32)[None, :]

    def enter(slot, mean, inv):
        def tile(i, carry):
            r0 = pl.multiple_of(slot * own + i * TILE, TILE)
            x = xs[pl.ds(r0, TILE), :].astype(F32)
            g = ((x - mean) * inv * gain + off).astype(BF16)
            hid = (dot(g, win[...]) + bin_ref[...].astype(F32)[None, :]).astype(BF16)
            hs[pl.ds(r0, TILE), :] = hid
            qkv_tile(hid, lng_ref[0, 0:1, :], lnb_ref[0, 0:1, :], wqkv0, slot, r0, pl.multiple_of(i * TILE, TILE), qs, k0, vt0)
            return carry
        return tile
    lax.fori_loop(0, sh_tiles, enter(1, mean_sh, inv_sh), 0)
    begin(kv_copies(0))

    def own_entry():
        locals_in[0].wait()
        for k in range(1, n):
            in_remote(0, lax.rem(me + k, n), me).wait_recv()
        count = float(own * group_ch)
        mean, m2 = column_stats(xs, 0, own, count, ind)
        lax.fori_loop(0, own_tiles, enter(0, mean, lax.rsqrt(m2 / count + 1e-6)), 0)

    for layer in range(layers):
        last = layer == layers - 1
        k_all, vt_all = ks[layer], vts[layer]
        loads = layer_loads(layer)
        if layer:
            begin(loads)
        for c in kv_copies(layer):
            c.wait_recv()

        def tile(it, carry):
            f = (it + own_tiles - sh_tiles) // own_tiles
            slot = 1 - f
            idx = f * lax.rem(chip + 1 + it + own_tiles - sh_tiles, own_tiles) + slot * (own_tiles + it)
            r0 = pl.multiple_of(idx * TILE, TILE)
            k0r = pl.multiple_of(idx * TILE - slot * own, TILE)
            if layer == 0:
                pl.when(it == sh_tiles)(own_entry)
            self_attend(slot, r0, qs, k_all, vt_all, s0, s1, ot, scale)

            @pl.when(it == 0)
            def _():
                finish(loads)
                if not last:
                    finish(qkv_loads(layer + 1))
            hid = (hs[pl.ds(r0, TILE), :].astype(F32) + dot(ot[...].T, wo[...]) + bself_ref[layer:layer + 1, :].astype(F32)).astype(BF16)
            qc = dot(layer_norm(hid, lng_ref[1, layer:layer + 1, :], lnb_ref[1, layer:layer + 1, :]), wcq[...]).astype(BF16)
            text_attend(layer, slot, qc, tk, tvt, ot, text_len, scale)
            hid = (hid.astype(F32) + dot(ot[...].T, wco[...]) + bcross_ref[layer:layer + 1, :].astype(F32)).astype(BF16)
            a = layer_norm(hid, lng_ref[2, layer:layer + 1, :], lnb_ref[2, layer:layer + 1, :])
            acc = None
            for c0 in range(0, ff, FF_CHUNK):
                pc, qcol = slice(c0, c0 + FF_CHUNK), slice(ff + c0, ff + c0 + FF_CHUNK)
                p = (dot(a, wff1[:, pc]) + bff1_ref[layer:layer + 1, pc].astype(F32)).astype(BF16).astype(F32)
                g = (dot(a, wff1[:, qcol]) + bff1_ref[layer:layer + 1, qcol].astype(F32)).astype(BF16).astype(F32)
                z = (p * (0.5 * g * (1.0 + lax.erf(g * math.sqrt(0.5))))).astype(BF16)
                prod = dot(z, wff2[pc, :])
                acc = prod if acc is None else acc + prod
            hid = (hid.astype(F32) + acc + bff2_ref[layer:layer + 1, :].astype(F32)).astype(BF16)
            if last:
                y = dot(hid, wout[...]) + bout_ref[...].astype(F32)[None, :] + xs[pl.ds(r0, TILE), :].astype(F32)
                xs[pl.ds(r0, TILE), :] = y.astype(BF16)

                @pl.when(slot == 0)
                def _():
                    for j in range(TILE // blk):
                        send_out(0, idx * (TILE // blk) + j)

                @pl.when(slot == 1)
                def _():
                    for j in range(TILE // part):
                        send_out(1, (idx - own_tiles) * (TILE // part) + j)
            else:
                hs[pl.ds(r0, TILE), :] = hid
                qkv_tile(hid, lng_ref[0, layer + 1:layer + 2, :], lnb_ref[0, layer + 1:layer + 2, :], wqkvs[layer + 1], slot, r0, k0r, qs,
                         ks[layer + 1], vts[layer + 1])

                @pl.when(it == sh_tiles - 1)
                def _():
                    begin(kv_copies(layer + 1))
            return carry
        lax.fori_loop(0, own_tiles + sh_tiles, tile, 0)

    for layer in range(layers):
        for c in kv_copies(layer):
            c.wait_send()
    for i in range(2):
        out_local(i).wait()
        for k in range(1, n):
            other = lax.rem(me + k, n)
            in_remote(i, me, other).wait_send()
            out_remote(i, me, other).wait_send()
            out_remote(i, other, me).wait_recv()


def solution(mesh):
    n = mesh.shape['sp']
    tok_spec = P('dp', 'sp', None, None)
    ctx_spec = P('dp', None, None)
    replicated = P()
    dma = pltpu.SemaphoreType.DMA

    def local_forward(latent, context, gn_gain, gn_bias, w_in, b_in, ln_gain, ln_bias, w_self, b_self, w_cross_q, w_cross_kv, w_cross_o, b_cross, w_ff1, b_ff1, w_ff2, b_ff2, w_out, b_out):
        batch, rows, columns, ch = latent.shape
        blk = rows * columns
        ff = w_ff2.shape[1]
        layers, text_len, text_dim = w_self.shape[0], context.shape[1], context.shape[2]
        per_chip = batch * CORES // n
        assert per_chip == CORES + 1 and layers == 2
        own = n * blk
        toks = own + own // CORES

        def vm(*dims, dtype=BF16):
            return pltpu.VMEM(dims, dtype)

        scratch = [
            vm(toks, ch), vm(toks, ch), vm(toks, ch), vm(2, own, ch), vm(2, own, ch), vm(2, ch, own), vm(2, ch, own),
            vm(own, TILE, dtype=F32), vm(own, TILE, dtype=F32), vm(ch, TILE),
            vm(layers, 2, TEXT_PAD, ch), vm(layers, 2, ch, TEXT_PAD), vm(TEXT_PAD, ch), vm(2, text_len, text_dim), vm(2, text_dim, ch),
            vm(ch, ch), vm(ch, ch), vm(ch, ch), vm(ch, ch), vm(ch, ch), vm(ch, 2 * ff), vm(ff, ch), vm(ch, 3 * ch), vm(ch, 3 * ch),
            vm(8, ch, dtype=F32), vm(8, ch, dtype=F32),
            dma((2, n)), dma((2, n)), dma((2, n)), dma((2, n)), dma((4,)), dma((2,)), dma((layers, 2)), dma((layers, 2)), dma((13,)), dma((2,)), dma((2,))]
        small = [gn_gain, gn_bias, b_in, ln_gain.transpose(1, 0, 2), ln_bias.transpose(1, 0, 2), b_self, b_cross, b_ff1, b_ff2, b_out]
        big = [latent.reshape(batch, blk, ch), context, w_in, w_self, w_cross_q, w_cross_kv, w_cross_o, w_ff1, w_ff2, w_out]
        out = pl.pallas_call(
            functools.partial(whole_kernel, n, per_chip, ch // NUM_GROUPS),
            out_shape=jax.ShapeDtypeStruct((batch, blk, ch), BF16),
            in_specs=[VMEM] * len(small) + [ANY] * len(big), out_specs=ANY, scratch_shapes=scratch,
            compiler_params=pltpu.CompilerParams(collective_id=0, has_side_effects=True, vmem_limit_bytes=62 * 1024 * 1024),
        )(*small, *big)
        return out.reshape(batch, rows, columns, ch)

    in_specs = (tok_spec, ctx_spec) + (replicated,) * 18
    return jax.shard_map(local_forward, mesh=mesh, in_specs=in_specs, out_specs=tok_spec, check_vma=False)
```

```python
import functools
import math

import jax
import jax.numpy as jnp
from jax import lax
from jax.experimental import pallas as pl
from jax.experimental.pallas import tpu as pltpu
from jax.sharding import PartitionSpec as P

HEAD_DIM = 64
NUM_GROUPS = 32
CORES = 2
TILE = 256
FF_CHUNK = 512
TEXT_PAD = 128
KEY_CHUNK = 512
LANES = 128
MESH = pl.DeviceIdType.MESH
F32 = jnp.float32
BF16 = jnp.bfloat16
ANY = pl.BlockSpec(memory_space=pl.ANY)
VMEM = pl.BlockSpec(memory_space=pltpu.VMEM)
NT = (((1,), (1,)), ((), ()))


def dot(a, b):
    return jnp.dot(a, b, preferred_element_type=F32)


def dot_nt(a, b):
    return lax.dot_general(a, b, NT, preferred_element_type=F32)


def layer_norm(hidden, gain, bias):
    vals = hidden.astype(F32)
    mean_val = jnp.mean(vals, axis=-1, keepdims=True)
    centered = vals - mean_val
    var_val = jnp.mean(centered * centered, axis=-1, keepdims=True)
    scaled = centered * lax.rsqrt(var_val + 1e-5)
    return (scaled * gain.astype(F32) + bias.astype(F32)).astype(BF16)


def entry_barrier(n):
    me = lax.axis_index('sp')
    sem = pltpu.get_barrier_semaphore()
    for k in range(1, n):
        pl.semaphore_signal(sem, inc=1, device_id={'sp': lax.rem(me + k, n)}, device_id_type=MESH)
    pl.semaphore_wait(sem, n - 1)


def group_sum(row, ind):
    hi = row.astype(BF16)
    rest = row - hi.astype(F32)
    mid = rest.astype(BF16)
    low = (rest - mid.astype(F32)).astype(BF16)
    total = None
    for piece in (low, mid, hi):
        term = dot(jnp.broadcast_to(piece, (16, piece.shape[1])), ind)[0:1]
        total = term if total is None else total + term
    return total


def same_group(ch, group_ch):
    def gid(axis):
        pos = lax.broadcasted_iota(jnp.int32, (ch, ch), axis).astype(F32)
        return jnp.floor((pos + 0.5) * (1.0 / group_ch))
    return jnp.where(gid(0) == gid(1), 1.0, 0.0).astype(BF16)


def column_stats(x_ref, lo, hi, count, ind):
    steps = (hi - lo) // TILE
    zero = jnp.zeros((1, x_ref.shape[1]), F32)

    def rows(i):
        return x_ref[pl.ds(pl.multiple_of(lo + i * TILE, TILE), TILE), :].astype(F32)

    mean = group_sum(lax.fori_loop(0, steps, lambda i, acc: acc + jnp.sum(rows(i), axis=0, keepdims=True), zero), ind) / count

    def sq(i, acc):
        d = rows(i) - mean
        return acc + jnp.sum(d * d, axis=0, keepdims=True)
    return mean, group_sum(lax.fori_loop(0, steps, sq, zero), ind)


def qkv_tile(hid, gain, bias, wqkv, slot, r0, k0, q_ref, k_ref, vt_ref):
    ch = hid.shape[1]
    a = layer_norm(hid, gain, bias)
    r = dot(a, wqkv[...]).astype(BF16)
    q_ref[pl.ds(r0, TILE), :] = r[:, :ch]
    k_ref[slot, pl.ds(k0, TILE), :] = r[:, ch:2 * ch]
    vt_ref[slot, :, pl.ds(k0, TILE)] = r[:, 2 * ch:].T


def head_mask(qp, half):
    lane = lax.broadcasted_iota(jnp.int32, qp.shape, 1)
    return jnp.where((lane >= HEAD_DIM) if half else (lane < HEAD_DIM), qp, jnp.zeros_like(qp))


def self_attend(slot, r0, q_ref, k_ref, vt_ref, s0, s1, ot, scale):
    keys, ch = k_ref.shape[1:]
    pairs = ch // LANES

    def step(cur, top, d0, nxt, pair, half):
        col = pl.multiple_of(pair * LANES, LANES)
        if nxt is not None:
            qm = head_mask(q_ref[pl.ds(r0, TILE), pl.ds(col, LANES)], half)
        new_top = total = acc = None
        for c in range(0, keys, KEY_CHUNK):
            rows = slice(c, c + KEY_CHUNK)
            if nxt is not None:
                s = dot_nt(k_ref[slot, rows, pl.ds(col, LANES)], qm)
                nxt[rows, :] = s
                peak = jnp.max(s, axis=0, keepdims=True)
                new_top = peak if new_top is None else jnp.maximum(new_top, peak)
            if cur is not None:
                p = jnp.exp2(cur[rows, :] * scale - top)
                part = jnp.sum(p, axis=0, keepdims=True)
                prod = dot(vt_ref[slot, pl.ds(d0, HEAD_DIM), rows], p.astype(BF16))
                total = part if total is None else total + part
                acc = prod if acc is None else acc + prod
        if cur is not None:
            ot[pl.ds(d0, HEAD_DIM), :] = (acc / total).astype(BF16)
        return None if nxt is None else new_top * scale

    def body(pair, top):
        d0 = pl.multiple_of(pair * LANES, LANES)
        top = step(s0, top, d0, s1, pair, 1)
        return step(s1, top, pl.multiple_of(d0 + HEAD_DIM, HEAD_DIM), s0, lax.rem(pair + 1, pairs), 0)

    lax.fori_loop(0, pairs, body, step(None, None, 0, s0, 0, 0))


def text_attend(layer, slot, qc, tk, tvt, ot, text_len, scale):
    ch = qc.shape[1]
    used = -(-text_len // 16) * 16
    heads = ch // HEAD_DIM
    scores = []
    for h in range(heads):
        cols = slice(h // 2 * LANES, (h // 2 + 1) * LANES)
        scores.append(dot_nt(tk[layer, slot, 0:used, cols], head_mask(qc[:, cols], h % 2)))
    keep = lax.broadcasted_iota(jnp.int32, scores[0].shape, 0) < text_len
    for h in range(heads):
        s = jnp.where(keep, scores[h], jnp.finfo(F32).min)
        top = jnp.max(s, axis=0, keepdims=True) * scale
        p = jnp.where(keep, jnp.exp2(s * scale - top), 0.0)
        total = jnp.sum(p, axis=0, keepdims=True)
        pb = jnp.concatenate([p.astype(BF16), jnp.zeros((TEXT_PAD - used, p.shape[1]), BF16)], axis=0)
        ot[h * HEAD_DIM:(h + 1) * HEAD_DIM, :] = (dot(tvt[layer, slot, h * HEAD_DIM:(h + 1) * HEAD_DIM, :], pb) / total).astype(BF16)


def whole_kernel(n, per_chip, group_ch,
                 gng_ref, gnb_ref, bin_ref, lng_ref, lnb_ref, bself_ref, bcross_ref, bff1_ref, bff2_ref, bout_ref,
                 x_ref, ctx_ref, win_ref, wself_ref, wcq_ref, wxkv_ref, wco_ref, wff1_ref, wff2_ref, wout_ref,
                 out_ref,
                 xs, hs, qs, k0, k1, vt0, vt1, s0, s1, ot, tk, tvt, vtmp, ctx, wx, win, wout, wo, wcq, wco, wff1, wff2, wqkv0, wqkv1,
                 st_mine, st_peer, in_send, in_recv, out_send, out_recv, local_sem, st_sem, kv_send, kv_recv, w_sem, c_sem, x_sem):
    me = lax.axis_index('sp')
    chip, core = me // CORES, lax.rem(me, CORES)
    peer = chip * CORES + (CORES - 1 - core)
    blk, ch = x_ref.shape[1:]
    part = blk // CORES
    own = n * blk
    rows = xs.shape[0]
    shared = rows - own
    ff = wff2.shape[0]
    text_len = ctx_ref.shape[1]
    own_tiles, sh_tiles = own // TILE, shared // TILE
    scale = HEAD_DIM ** -0.5 * math.log2(math.e)
    ks, vts, wqkvs = (k0, k1), (vt0, vt1), (wqkv0, wqkv1)
    layers = wself_ref.shape[0]

    ctx_loads = [pltpu.make_async_copy(ctx_ref.at[chip * per_chip + core], ctx.at[0], c_sem.at[0]),
                 pltpu.make_async_copy(ctx_ref.at[chip * per_chip + CORES], ctx.at[1], c_sem.at[1])]

    def text_loads(layer):
        return [pltpu.make_async_copy(wxkv_ref.at[layer, j], wx.at[j], x_sem.at[j]) for j in range(2)]

    def qkv_loads(layer):
        return [pltpu.make_async_copy(wself_ref.at[layer, j], wqkvs[layer].at[:, pl.ds(j * ch, ch)], w_sem.at[10 * layer + j]) for j in range(3)]

    def layer_loads(layer):
        pairs = ((wself_ref.at[layer, 3], wo), (wcq_ref.at[layer], wcq), (wco_ref.at[layer], wco), (wff1_ref.at[layer], wff1), (wff2_ref.at[layer], wff2))
        return [pltpu.make_async_copy(src, dst, w_sem.at[3 + j]) for j, (src, dst) in enumerate(pairs)]

    edge_loads = [pltpu.make_async_copy(win_ref, win, w_sem.at[8]), pltpu.make_async_copy(wout_ref, wout, w_sem.at[9])]

    def begin(copies):
        for c in copies:
            c.start()

    def finish(copies):
        for c in copies:
            c.wait()

    def in_copy(i, src, dest):
        to_chip, to_core = dest // CORES, lax.rem(dest, CORES)
        source = (x_ref.at[to_chip * per_chip + to_core],
                  x_ref.at[to_chip * per_chip + CORES, pl.ds(pl.multiple_of(to_core * part, part), part)])[i]
        target = (xs.at[pl.ds(pl.multiple_of(src * blk, blk), blk)],
                  xs.at[pl.ds(pl.multiple_of(own + src * part, part), part)])[i]
        return source, target

    def in_remote(i, src, dest):
        source, target = in_copy(i, src, dest)
        return pltpu.make_async_remote_copy(
            src_ref=source, dst_ref=target, send_sem=in_send.at[i, dest], recv_sem=in_recv.at[i, src],
            device_id={'sp': dest}, device_id_type=MESH)

    def out_copy(i, src, dest):
        from_chip, from_core = src // CORES, lax.rem(src, CORES)
        source = (xs.at[pl.ds(pl.multiple_of(dest * blk, blk), blk)],
                  xs.at[pl.ds(pl.multiple_of(own + dest * part, part), part)])[i]
        target = (out_ref.at[from_chip * per_chip + from_core],
                  out_ref.at[from_chip * per_chip + CORES, pl.ds(pl.multiple_of(from_core * part, part), part)])[i]
        return source, target

    def out_remote(i, src, dest):
        source, target = out_copy(i, src, dest)
        return pltpu.make_async_remote_copy(
            src_ref=source, dst_ref=target, send_sem=out_send.at[i, dest], recv_sem=out_recv.at[i, src],
            device_id={'sp': dest}, device_id_type=MESH)

    def out_local(i):
        source, target = out_copy(i, me, me)
        return pltpu.make_async_copy(source, target, local_sem.at[2 + i])

    def send_out(i, dest):
        @pl.when(dest != me)
        def _():
            out_remote(i, me, dest).start()

        @pl.when(dest == me)
        def _():
            out_local(i).start()

    def kv_copies(layer):
        k, vt = ks[layer], vts[layer]
        args = ((k.at[1, pl.ds(0, shared)], k.at[1, pl.ds(shared, shared)]),
                (vt.at[1, :, pl.ds(0, shared)], vt.at[1, :, pl.ds(shared, shared)]))
        return [pltpu.make_async_remote_copy(
            src_ref=a, dst_ref=b, send_sem=kv_send.at[layer, j], recv_sem=kv_recv.at[layer, j],
            device_id={'sp': peer}, device_id_type=MESH) for j, (a, b) in enumerate(args)]

    begin(ctx_loads)
    begin(text_loads(0))
    locals_in = [pltpu.make_async_copy(*in_copy(i, me, me), local_sem.at[i]) for i in range(2)]
    begin(locals_in)
    entry_barrier(n)
    for i in (1, 0):
        for k in range(1, n):
            in_remote(i, me, lax.rem(me + k, n)).start()
    begin(edge_loads)
    begin(qkv_loads(0))

    tk[...] = jnp.zeros_like(tk)
    vtmp[...] = jnp.zeros_like(vtmp)
    finish(ctx_loads)
    for layer in range(layers):
        finish(text_loads(layer))
        for s in range(2):
            tk[layer, s, 0:text_len, :] = dot(ctx[s], wx[0]).astype(BF16)
            vtmp[0:text_len, :] = dot(ctx[s], wx[1]).astype(BF16)
            tvt[layer, s] = vtmp[...].T
        if layer + 1 < layers:
            begin(text_loads(layer + 1))
    begin(layer_loads(0))
    begin(qkv_loads(1))
    ind = same_group(ch, group_ch)

    locals_in[1].wait()
    for k in range(1, n):
        in_remote(1, lax.rem(me + k, n), me).wait_recv()
    half = float(shared * group_ch)
    mean, m2 = column_stats(xs, own, rows, half, ind)
    st_mine[...] = jnp.zeros_like(st_mine)
    st_mine[0:1, :] = mean
    st_mine[1:2, :] = m2
    st_copy = pltpu.make_async_remote_copy(
        src_ref=st_mine, dst_ref=st_peer, send_sem=st_sem.at[0], recv_sem=st_sem.at[1], device_id={'sp': peer}, device_id_type=MESH)
    st_copy.start()
    finish(edge_loads)
    finish(qkv_loads(0))
    st_copy.wait()
    delta = mean - st_peer[0:1, :]
    mean_sh = (mean + st_peer[0:1, :]) * 0.5
    m2 = m2 + st_peer[1:2, :] + delta * delta * (half * 0.5)
    inv_sh = lax.rsqrt(m2 / (2.0 * half) + 1e-6)
    gain = gng_ref[...].astype(F32)[None, :]
    off = gnb_ref[...].astype(F32)[None, :]

    def enter(slot, mean, inv):
        def tile(i, carry):
            r0 = pl.multiple_of(slot * own + i * TILE, TILE)
            x = xs[pl.ds(r0, TILE), :].astype(F32)
            g = ((x - mean) * inv * gain + off).astype(BF16)
            hid = (dot(g, win[...]) + bin_ref[...].astype(F32)[None, :]).astype(BF16)
            hs[pl.ds(r0, TILE), :] = hid
            qkv_tile(hid, lng_ref[0, 0:1, :], lnb_ref[0, 0:1, :], wqkv0, slot, r0, pl.multiple_of(i * TILE, TILE), qs, k0, vt0)
            return carry
        return tile
    lax.fori_loop(0, sh_tiles, enter(1, mean_sh, inv_sh), 0)
    begin(kv_copies(0))

    def own_entry():
        locals_in[0].wait()
        for k in range(1, n):
            in_remote(0, lax.rem(me + k, n), me).wait_recv()
        count = float(own * group_ch)
        mean, m2 = column_stats(xs, 0, own, count, ind)
        lax.fori_loop(0, own_tiles, enter(0, mean, lax.rsqrt(m2 / count + 1e-6)), 0)

    for layer in range(layers):
        last = layer == layers - 1
        k_all, vt_all = ks[layer], vts[layer]
        loads = layer_loads(layer)
        if layer:
            begin(loads)
        for c in kv_copies(layer):
            c.wait_recv()

        def tile(it, carry):
            f = (it + own_tiles - sh_tiles) // own_tiles
            slot = 1 - f
            idx = f * lax.rem(chip + 1 + it + own_tiles - sh_tiles, own_tiles) + slot * (own_tiles + it)
            r0 = pl.multiple_of(idx * TILE, TILE)
            k0r = pl.multiple_of(idx * TILE - slot * own, TILE)
            if layer == 0:
                pl.when(it == sh_tiles)(own_entry)
            self_attend(slot, r0, qs, k_all, vt_all, s0, s1, ot, scale)

            @pl.when(it == 0)
            def _():
                finish(loads)
                if not last:
                    finish(qkv_loads(layer + 1))
            hid = (hs[pl.ds(r0, TILE), :].astype(F32) + dot(ot[...].T, wo[...]) + bself_ref[layer:layer + 1, :].astype(F32)).astype(BF16)
            qc = dot(layer_norm(hid, lng_ref[1, layer:layer + 1, :], lnb_ref[1, layer:layer + 1, :]), wcq[...]).astype(BF16)
            text_attend(layer, slot, qc, tk, tvt, ot, text_len, scale)
            hid = (hid.astype(F32) + dot(ot[...].T, wco[...]) + bcross_ref[layer:layer + 1, :].astype(F32)).astype(BF16)
            a = layer_norm(hid, lng_ref[2, layer:layer + 1, :], lnb_ref[2, layer:layer + 1, :])
            acc = None
            for c0 in range(0, ff, FF_CHUNK):
                pc, qcol = slice(c0, c0 + FF_CHUNK), slice(ff + c0, ff + c0 + FF_CHUNK)
                p = (dot(a, wff1[:, pc]) + bff1_ref[layer:layer + 1, pc].astype(F32)).astype(BF16).astype(F32)
                g = (dot(a, wff1[:, qcol]) + bff1_ref[layer:layer + 1, qcol].astype(F32)).astype(BF16).astype(F32)
                z = (p * (0.5 * g * (1.0 + lax.erf(g * math.sqrt(0.5))))).astype(BF16)
                prod = dot(z, wff2[pc, :])
                acc = prod if acc is None else acc + prod
            hid = (hid.astype(F32) + acc + bff2_ref[layer:layer + 1, :].astype(F32)).astype(BF16)
            if last:
                y = dot(hid, wout[...]) + bout_ref[...].astype(F32)[None, :] + xs[pl.ds(r0, TILE), :].astype(F32)
                xs[pl.ds(r0, TILE), :] = y.astype(BF16)

                @pl.when(slot == 0)
                def _():
                    for j in range(TILE // blk):
                        send_out(0, idx * (TILE // blk) + j)

                @pl.when(slot == 1)
                def _():
                    for j in range(TILE // part):
                        send_out(1, (idx - own_tiles) * (TILE // part) + j)
            else:
                hs[pl.ds(r0, TILE), :] = hid
                qkv_tile(hid, lng_ref[0, layer + 1:layer + 2, :], lnb_ref[0, layer + 1:layer + 2, :], wqkvs[layer + 1], slot, r0, k0r, qs,
                         ks[layer + 1], vts[layer + 1])

                @pl.when(it == sh_tiles - 1)
                def _():
                    begin(kv_copies(layer + 1))
            return carry
        lax.fori_loop(0, own_tiles + sh_tiles, tile, 0)

    for layer in range(layers):
        for c in kv_copies(layer):
            c.wait_send()
    for i in range(2):
        out_local(i).wait()
        for k in range(1, n):
            other = lax.rem(me + k, n)
            in_remote(i, me, other).wait_send()
            out_remote(i, me, other).wait_send()
            out_remote(i, other, me).wait_recv()


def solution(mesh):
    n = mesh.shape['sp']
    tok_spec = P('dp', 'sp', None, None)
    ctx_spec = P('dp', None, None)
    replicated = P()
    dma = pltpu.SemaphoreType.DMA

    def local_forward(latent, context, gn_gain, gn_bias, w_in, b_in, ln_gain, ln_bias, w_self, b_self, w_cross_q, w_cross_kv, w_cross_o, b_cross, w_ff1, b_ff1, w_ff2, b_ff2, w_out, b_out):
        batch, rows, columns, ch = latent.shape
        blk = rows * columns
        ff = w_ff2.shape[1]
        layers, text_len, text_dim = w_self.shape[0], context.shape[1], context.shape[2]
        per_chip = batch * CORES // n
        assert per_chip == CORES + 1 and layers == 2
        own = n * blk
        toks = own + own // CORES

        def vm(*dims, dtype=BF16):
            return pltpu.VMEM(dims, dtype)

        scratch = [
            vm(toks, ch), vm(toks, ch), vm(toks, ch), vm(2, own, ch), vm(2, own, ch), vm(2, ch, own), vm(2, ch, own),
            vm(own, TILE, dtype=F32), vm(own, TILE, dtype=F32), vm(ch, TILE),
            vm(layers, 2, TEXT_PAD, ch), vm(layers, 2, ch, TEXT_PAD), vm(TEXT_PAD, ch), vm(2, text_len, text_dim), vm(2, text_dim, ch),
            vm(ch, ch), vm(ch, ch), vm(ch, ch), vm(ch, ch), vm(ch, ch), vm(ch, 2 * ff), vm(ff, ch), vm(ch, 3 * ch), vm(ch, 3 * ch),
            vm(8, ch, dtype=F32), vm(8, ch, dtype=F32),
            dma((2, n)), dma((2, n)), dma((2, n)), dma((2, n)), dma((4,)), dma((2,)), dma((layers, 2)), dma((layers, 2)), dma((13,)), dma((2,)), dma((2,))]
        small = [gn_gain, gn_bias, b_in, ln_gain.transpose(1, 0, 2), ln_bias.transpose(1, 0, 2), b_self, b_cross, b_ff1, b_ff2, b_out]
        big = [latent.reshape(batch, blk, ch), context, w_in, w_self, w_cross_q, w_cross_kv, w_cross_o, w_ff1, w_ff2, w_out]
        out = pl.pallas_call(
            functools.partial(whole_kernel, n, per_chip, ch // NUM_GROUPS),
            out_shape=jax.ShapeDtypeStruct((batch, blk, ch), BF16),
            in_specs=[VMEM] * len(small) + [ANY] * len(big), out_specs=ANY, scratch_shapes=scratch,
            compiler_params=pltpu.CompilerParams(collective_id=0, has_side_effects=True, vmem_limit_bytes=62 * 1024 * 1024),
        )(*small, *big)
        return out.reshape(batch, rows, columns, ch)

    in_specs = (tok_spec, ctx_spec) + (replicated,) * 18
    return jax.shard_map(local_forward, mesh=mesh, in_specs=in_specs, out_specs=tok_spec, check_vma=False)
```

```python
import functools
import math

import jax
import jax.numpy as jnp
from jax import lax
from jax.experimental import pallas as pl
from jax.experimental.pallas import tpu as pltpu
from jax.sharding import PartitionSpec as P

HEAD_DIM = 64
NUM_GROUPS = 32
CORES = 2
TILE = 256
FF_CHUNK = 512
TEXT_PAD = 128
KEY_CHUNK = 512
LANES = 128
MESH = pl.DeviceIdType.MESH
F32 = jnp.float32
BF16 = jnp.bfloat16
ANY = pl.BlockSpec(memory_space=pl.ANY)
VMEM = pl.BlockSpec(memory_space=pltpu.VMEM)
NT = (((1,), (1,)), ((), ()))


def dot(a, b):
    return jnp.dot(a, b, preferred_element_type=F32)


def dot_nt(a, b):
    return lax.dot_general(a, b, NT, preferred_element_type=F32)


def layer_norm(hidden, gain, bias):
    vals = hidden.astype(F32)
    mean_val = jnp.mean(vals, axis=-1, keepdims=True)
    centered = vals - mean_val
    var_val = jnp.mean(centered * centered, axis=-1, keepdims=True)
    scaled = centered * lax.rsqrt(var_val + 1e-5)
    return (scaled * gain.astype(F32) + bias.astype(F32)).astype(BF16)


def entry_barrier(n):
    me = lax.axis_index('sp')
    sem = pltpu.get_barrier_semaphore()
    for k in range(1, n):
        pl.semaphore_signal(sem, inc=1, device_id={'sp': lax.rem(me + k, n)}, device_id_type=MESH)
    pl.semaphore_wait(sem, n - 1)


def group_sum(row, ind):
    hi = row.astype(BF16)
    rest = row - hi.astype(F32)
    mid = rest.astype(BF16)
    low = (rest - mid.astype(F32)).astype(BF16)
    total = None
    for piece in (low, mid, hi):
        term = dot(jnp.broadcast_to(piece, (16, piece.shape[1])), ind)[0:1]
        total = term if total is None else total + term
    return total


def same_group(ch, group_ch):
    def gid(axis):
        pos = lax.broadcasted_iota(jnp.int32, (ch, ch), axis).astype(F32)
        return jnp.floor((pos + 0.5) * (1.0 / group_ch))
    return jnp.where(gid(0) == gid(1), 1.0, 0.0).astype(BF16)


def column_stats(x_ref, lo, hi, count, ind):
    steps = (hi - lo) // TILE
    zero = jnp.zeros((1, x_ref.shape[1]), F32)

    def rows(i):
        return x_ref[pl.ds(pl.multiple_of(lo + i * TILE, TILE), TILE), :].astype(F32)

    mean = group_sum(lax.fori_loop(0, steps, lambda i, acc: acc + jnp.sum(rows(i), axis=0, keepdims=True), zero), ind) / count

    def sq(i, acc):
        d = rows(i) - mean
        return acc + jnp.sum(d * d, axis=0, keepdims=True)
    return mean, group_sum(lax.fori_loop(0, steps, sq, zero), ind)


def qkv_tile(hid, gain, bias, wqkv, slot, r0, k0, q_ref, k_ref, vt_ref):
    ch = hid.shape[1]
    a = layer_norm(hid, gain, bias)
    r = dot(a, wqkv[...]).astype(BF16)
    q_ref[pl.ds(r0, TILE), :] = r[:, :ch]
    k_ref[slot, pl.ds(k0, TILE), :] = r[:, ch:2 * ch]
    vt_ref[slot, :, pl.ds(k0, TILE)] = r[:, 2 * ch:].T


def head_mask(qp, half):
    lane = lax.broadcasted_iota(jnp.int32, qp.shape, 1)
    return jnp.where((lane >= HEAD_DIM) if half else (lane < HEAD_DIM), qp, jnp.zeros_like(qp))


def self_attend(slot, r0, q_ref, k_ref, vt_ref, s0, s1, ot, scale):
    keys, ch = k_ref.shape[1:]
    pairs = ch // LANES

    def step(cur, top, d0, nxt, pair, half):
        col = pl.multiple_of(pair * LANES, LANES)
        if nxt is not None:
            qm = head_mask(q_ref[pl.ds(r0, TILE), pl.ds(col, LANES)], half)
        new_top = total = acc = None
        for c in range(0, keys, KEY_CHUNK):
            rows = slice(c, c + KEY_CHUNK)
            if nxt is not None:
                s = dot_nt(k_ref[slot, rows, pl.ds(col, LANES)], qm)
                nxt[rows, :] = s
                peak = jnp.max(s, axis=0, keepdims=True)
                new_top = peak if new_top is None else jnp.maximum(new_top, peak)
            if cur is not None:
                p = jnp.exp2(cur[rows, :] * scale - top)
                part = jnp.sum(p, axis=0, keepdims=True)
                prod = dot(vt_ref[slot, pl.ds(d0, HEAD_DIM), rows], p.astype(BF16))
                total = part if total is None else total + part
                acc = prod if acc is None else acc + prod
        if cur is not None:
            ot[pl.ds(d0, HEAD_DIM), :] = (acc / total).astype(BF16)
        return None if nxt is None else new_top * scale

    def body(pair, top):
        d0 = pl.multiple_of(pair * LANES, LANES)
        top = step(s0, top, d0, s1, pair, 1)
        return step(s1, top, pl.multiple_of(d0 + HEAD_DIM, HEAD_DIM), s0, lax.rem(pair + 1, pairs), 0)

    lax.fori_loop(0, pairs, body, step(None, None, 0, s0, 0, 0))


def text_attend(layer, slot, qc, tk, tvt, ot, text_len, scale):
    ch = qc.shape[1]
    used = -(-text_len // 16) * 16
    heads = ch // HEAD_DIM
    scores = []
    for h in range(heads):
        cols = slice(h // 2 * LANES, (h // 2 + 1) * LANES)
        scores.append(dot_nt(tk[layer, slot, 0:used, cols], head_mask(qc[:, cols], h % 2)))
    keep = lax.broadcasted_iota(jnp.int32, scores[0].shape, 0) < text_len
    for h in range(heads):
        s = jnp.where(keep, scores[h], jnp.finfo(F32).min)
        top = jnp.max(s, axis=0, keepdims=True) * scale
        p = jnp.where(keep, jnp.exp2(s * scale - top), 0.0)
        total = jnp.sum(p, axis=0, keepdims=True)
        pb = jnp.concatenate([p.astype(BF16), jnp.zeros((TEXT_PAD - used, p.shape[1]), BF16)], axis=0)
        ot[h * HEAD_DIM:(h + 1) * HEAD_DIM, :] = (dot(tvt[layer, slot, h * HEAD_DIM:(h + 1) * HEAD_DIM, :], pb) / total).astype(BF16)


def whole_kernel(n, per_chip, group_ch,
                 gng_ref, gnb_ref, bin_ref, lng_ref, lnb_ref, bself_ref, bcross_ref, bff1_ref, bff2_ref, bout_ref,
                 x_ref, ctx_ref, win_ref, wself_ref, wcq_ref, wxkv_ref, wco_ref, wff1_ref, wff2_ref, wout_ref,
                 out_ref,
                 xs, hs, qs, k0, k1, vt0, vt1, s0, s1, ot, tk, tvt, vtmp, ctx, wx, win, wout, wo2, wcq2, wco2, wff12, wff22, wqkv0, wqkv1,
                 st_mine, st_peer, in_send, in_recv, out_send, out_recv, local_sem, st_sem, kv_send, kv_recv, w_sem, c_sem, x_sem):
    me = lax.axis_index('sp')
    chip, core = me // CORES, lax.rem(me, CORES)
    peer = chip * CORES + (CORES - 1 - core)
    blk, ch = x_ref.shape[1:]
    part = blk // CORES
    own = n * blk
    rows = xs.shape[0]
    shared = rows - own
    ff = wff22.shape[1]
    text_len = ctx_ref.shape[1]
    own_tiles, sh_tiles = own // TILE, shared // TILE
    scale = HEAD_DIM ** -0.5 * math.log2(math.e)
    ks, vts, wqkvs = (k0, k1), (vt0, vt1), (wqkv0, wqkv1)
    layers = wself_ref.shape[0]

    ctx_loads = [pltpu.make_async_copy(ctx_ref.at[chip * per_chip + core], ctx.at[0], c_sem.at[0]),
                 pltpu.make_async_copy(ctx_ref.at[chip * per_chip + CORES], ctx.at[1], c_sem.at[1])]

    def text_loads(layer):
        return [pltpu.make_async_copy(wxkv_ref.at[layer, j], wx.at[j], x_sem.at[j]) for j in range(2)]

    def qkv_loads(layer):
        return [pltpu.make_async_copy(wself_ref.at[layer, j], wqkvs[layer].at[:, pl.ds(j * ch, ch)], w_sem.at[10 * layer + j]) for j in range(3)]

    def layer_loads(layer):
        pairs = ((wself_ref.at[layer, 3], wo2), (wcq_ref.at[layer], wcq2), (wco_ref.at[layer], wco2), (wff1_ref.at[layer], wff12), (wff2_ref.at[layer], wff22))
        return [pltpu.make_async_copy(src, dst.at[layer], w_sem.at[13 + 5 * layer + j]) for j, (src, dst) in enumerate(pairs)]

    edge_loads = [pltpu.make_async_copy(win_ref, win, w_sem.at[8]), pltpu.make_async_copy(wout_ref, wout, w_sem.at[9])]

    def begin(copies):
        for c in copies:
            c.start()

    def finish(copies):
        for c in copies:
            c.wait()

    def in_copy(i, src, dest):
        to_chip, to_core = dest // CORES, lax.rem(dest, CORES)
        source = (x_ref.at[to_chip * per_chip + to_core],
                  x_ref.at[to_chip * per_chip + CORES, pl.ds(pl.multiple_of(to_core * part, part), part)])[i]
        target = (xs.at[pl.ds(pl.multiple_of(src * blk, blk), blk)],
                  xs.at[pl.ds(pl.multiple_of(own + src * part, part), part)])[i]
        return source, target

    def in_remote(i, src, dest):
        source, target = in_copy(i, src, dest)
        return pltpu.make_async_remote_copy(
            src_ref=source, dst_ref=target, send_sem=in_send.at[i, dest], recv_sem=in_recv.at[i, src],
            device_id={'sp': dest}, device_id_type=MESH)

    def out_copy(i, src, dest):
        from_chip, from_core = src // CORES, lax.rem(src, CORES)
        source = (xs.at[pl.ds(pl.multiple_of(dest * blk, blk), blk)],
                  xs.at[pl.ds(pl.multiple_of(own + dest * part, part), part)])[i]
        target = (out_ref.at[from_chip * per_chip + from_core],
                  out_ref.at[from_chip * per_chip + CORES, pl.ds(pl.multiple_of(from_core * part, part), part)])[i]
        return source, target

    def out_remote(i, src, dest):
        source, target = out_copy(i, src, dest)
        return pltpu.make_async_remote_copy(
            src_ref=source, dst_ref=target, send_sem=out_send.at[i, dest], recv_sem=out_recv.at[i, src],
            device_id={'sp': dest}, device_id_type=MESH)

    def out_local(i):
        source, target = out_copy(i, me, me)
        return pltpu.make_async_copy(source, target, local_sem.at[2 + i])

    def send_out(i, dest):
        @pl.when(dest != me)
        def _():
            out_remote(i, me, dest).start()

        @pl.when(dest == me)
        def _():
            out_local(i).start()

    def kv_copies(layer):
        k, vt = ks[layer], vts[layer]
        args = ((k.at[1, pl.ds(0, shared)], k.at[1, pl.ds(shared, shared)]),
                (vt.at[1, :, pl.ds(0, shared)], vt.at[1, :, pl.ds(shared, shared)]))
        return [pltpu.make_async_remote_copy(
            src_ref=a, dst_ref=b, send_sem=kv_send.at[layer, j], recv_sem=kv_recv.at[layer, j],
            device_id={'sp': peer}, device_id_type=MESH) for j, (a, b) in enumerate(args)]

    begin(ctx_loads)
    begin(text_loads(0))
    locals_in = [pltpu.make_async_copy(*in_copy(i, me, me), local_sem.at[i]) for i in range(2)]
    begin(locals_in)
    entry_barrier(n)
    for k in range(1, n):
        in_remote(1, me, lax.rem(me + k, n)).start()
    begin(edge_loads)
    begin(qkv_loads(0))

    tk[...] = jnp.zeros_like(tk)
    vtmp[...] = jnp.zeros_like(vtmp)
    finish(ctx_loads)

    def text_keys(layer):
        finish(text_loads(layer))
        for s in range(2):
            tk[layer, s, 0:text_len, :] = dot(ctx[s], wx[0]).astype(BF16)
            vtmp[0:text_len, :] = dot(ctx[s], wx[1]).astype(BF16)
            tvt[layer, s] = vtmp[...].T

    text_keys(0)
    for k in range(1, n):
        in_remote(1, me, lax.rem(me + k, n)).wait_send()
    for k in range(1, n):
        in_remote(0, me, lax.rem(me + k, n)).start()
    begin(text_loads(1))
    begin(layer_loads(0))
    begin(qkv_loads(1))
    begin(layer_loads(1))
    ind = same_group(ch, group_ch)

    locals_in[1].wait()
    for k in range(1, n):
        in_remote(1, lax.rem(me + k, n), me).wait_recv()
    half = float(shared * group_ch)
    mean, m2 = column_stats(xs, own, rows, half, ind)
    st_mine[...] = jnp.zeros_like(st_mine)
    st_mine[0:1, :] = mean
    st_mine[1:2, :] = m2
    st_copy = pltpu.make_async_remote_copy(
        src_ref=st_mine, dst_ref=st_peer, send_sem=st_sem.at[0], recv_sem=st_sem.at[1], device_id={'sp': peer}, device_id_type=MESH)
    st_copy.start()
    finish(edge_loads)
    finish(qkv_loads(0))
    st_copy.wait()
    delta = mean - st_peer[0:1, :]
    mean_sh = (mean + st_peer[0:1, :]) * 0.5
    m2 = m2 + st_peer[1:2, :] + delta * delta * (half * 0.5)
    inv_sh = lax.rsqrt(m2 / (2.0 * half) + 1e-6)
    gain = gng_ref[...].astype(F32)[None, :]
    off = gnb_ref[...].astype(F32)[None, :]

    def enter(slot, mean, inv):
        def tile(i, carry):
            r0 = pl.multiple_of(slot * own + i * TILE, TILE)
            x = xs[pl.ds(r0, TILE), :].astype(F32)
            g = ((x - mean) * inv * gain + off).astype(BF16)
            hid = (dot(g, win[...]) + bin_ref[...].astype(F32)[None, :]).astype(BF16)
            hs[pl.ds(r0, TILE), :] = hid
            qkv_tile(hid, lng_ref[0, 0:1, :], lnb_ref[0, 0:1, :], wqkv0, slot, r0, pl.multiple_of(i * TILE, TILE), qs, k0, vt0)
            return carry
        return tile
    lax.fori_loop(0, sh_tiles, enter(1, mean_sh, inv_sh), 0)
    begin(kv_copies(0))
    text_keys(1)

    def own_entry():
        locals_in[0].wait()
        for k in range(1, n):
            in_remote(0, lax.rem(me + k, n), me).wait_recv()
        count = float(own * group_ch)
        mean, m2 = column_stats(xs, 0, own, count, ind)
        lax.fori_loop(0, own_tiles, enter(0, mean, lax.rsqrt(m2 / count + 1e-6)), 0)

    for layer in range(layers):
        last = layer == layers - 1
        k_all, vt_all = ks[layer], vts[layer]
        loads = layer_loads(layer)
        wo, wcq, wco, wff1, wff2 = (w.at[layer] for w in (wo2, wcq2, wco2, wff12, wff22))
        for c in kv_copies(layer):
            c.wait_recv()

        def tile(it, carry):
            f = (it + own_tiles - sh_tiles) // own_tiles
            slot = 1 - f
            idx = f * lax.rem(chip + 1 + it + own_tiles - sh_tiles, own_tiles) + slot * (own_tiles + it)
            r0 = pl.multiple_of(idx * TILE, TILE)
            k0r = pl.multiple_of(idx * TILE - slot * own, TILE)
            if layer == 0:
                pl.when(it == sh_tiles)(own_entry)
            self_attend(slot, r0, qs, k_all, vt_all, s0, s1, ot, scale)

            @pl.when(it == 0)
            def _():
                finish(loads)
                if not last:
                    finish(qkv_loads(layer + 1))
            hid = (hs[pl.ds(r0, TILE), :].astype(F32) + dot(ot[...].T, wo[...]) + bself_ref[layer:layer + 1, :].astype(F32)).astype(BF16)
            qc = dot(layer_norm(hid, lng_ref[1, layer:layer + 1, :], lnb_ref[1, layer:layer + 1, :]), wcq[...]).astype(BF16)
            text_attend(layer, slot, qc, tk, tvt, ot, text_len, scale)
            hid = (hid.astype(F32) + dot(ot[...].T, wco[...]) + bcross_ref[layer:layer + 1, :].astype(F32)).astype(BF16)
            a = layer_norm(hid, lng_ref[2, layer:layer + 1, :], lnb_ref[2, layer:layer + 1, :])
            acc = None
            for c0 in range(0, ff, FF_CHUNK):
                pc, qcol = slice(c0, c0 + FF_CHUNK), slice(ff + c0, ff + c0 + FF_CHUNK)
                p = (dot(a, wff1[:, pc]) + bff1_ref[layer:layer + 1, pc].astype(F32)).astype(BF16).astype(F32)
                g = (dot(a, wff1[:, qcol]) + bff1_ref[layer:layer + 1, qcol].astype(F32)).astype(BF16).astype(F32)
                z = (p * (0.5 * g * (1.0 + lax.erf(g * math.sqrt(0.5))))).astype(BF16)
                prod = dot(z, wff2[pc, :])
                acc = prod if acc is None else acc + prod
            hid = (hid.astype(F32) + acc + bff2_ref[layer:layer + 1, :].astype(F32)).astype(BF16)
            if last:
                y = dot(hid, wout[...]) + bout_ref[...].astype(F32)[None, :] + xs[pl.ds(r0, TILE), :].astype(F32)
                xs[pl.ds(r0, TILE), :] = y.astype(BF16)

                @pl.when(slot == 0)
                def _():
                    for j in range(TILE // blk):
                        send_out(0, idx * (TILE // blk) + j)

                @pl.when(slot == 1)
                def _():
                    for j in range(TILE // part):
                        send_out(1, (idx - own_tiles) * (TILE // part) + j)
            else:
                hs[pl.ds(r0, TILE), :] = hid
                qkv_tile(hid, lng_ref[0, layer + 1:layer + 2, :], lnb_ref[0, layer + 1:layer + 2, :], wqkvs[layer + 1], slot, r0, k0r, qs,
                         ks[layer + 1], vts[layer + 1])

                @pl.when(it == sh_tiles - 1)
                def _():
                    begin(kv_copies(layer + 1))
            return carry
        lax.fori_loop(0, own_tiles + sh_tiles, tile, 0)

    for layer in range(layers):
        for c in kv_copies(layer):
            c.wait_send()
    for i in range(2):
        out_local(i).wait()
        for k in range(1, n):
            other = lax.rem(me + k, n)
            if i == 0:
                in_remote(i, me, other).wait_send()
            out_remote(i, me, other).wait_send()
            out_remote(i, other, me).wait_recv()


def solution(mesh):
    n = mesh.shape['sp']
    tok_spec = P('dp', 'sp', None, None)
    ctx_spec = P('dp', None, None)
    replicated = P()
    dma = pltpu.SemaphoreType.DMA

    def local_forward(latent, context, gn_gain, gn_bias, w_in, b_in, ln_gain, ln_bias, w_self, b_self, w_cross_q, w_cross_kv, w_cross_o, b_cross, w_ff1, b_ff1, w_ff2, b_ff2, w_out, b_out):
        batch, rows, columns, ch = latent.shape
        blk = rows * columns
        ff = w_ff2.shape[1]
        layers, text_len, text_dim = w_self.shape[0], context.shape[1], context.shape[2]
        per_chip = batch * CORES // n
        assert per_chip == CORES + 1 and layers == 2
        own = n * blk
        toks = own + own // CORES

        def vm(*dims, dtype=BF16):
            return pltpu.VMEM(dims, dtype)

        scratch = [
            vm(toks, ch), vm(toks, ch), vm(toks, ch), vm(2, own, ch), vm(2, own, ch), vm(2, ch, own), vm(2, ch, own),
            vm(own, TILE, dtype=F32), vm(own, TILE, dtype=F32), vm(ch, TILE),
            vm(layers, 2, TEXT_PAD, ch), vm(layers, 2, ch, TEXT_PAD), vm(TEXT_PAD, ch), vm(2, text_len, text_dim), vm(2, text_dim, ch),
            vm(ch, ch), vm(ch, ch), vm(layers, ch, ch), vm(layers, ch, ch), vm(layers, ch, ch), vm(layers, ch, 2 * ff), vm(layers, ff, ch), vm(ch, 3 * ch), vm(ch, 3 * ch),
            vm(32, ch, dtype=F32), vm(32, ch, dtype=F32),
            dma((2, n)), dma((2, n)), dma((2, n)), dma((2, n)), dma((4,)), dma((2,)), dma((layers, 2)), dma((layers, 2)), dma((23,)), dma((2,)), dma((2,))]
        small = [gn_gain, gn_bias, b_in, ln_gain.transpose(1, 0, 2), ln_bias.transpose(1, 0, 2), b_self, b_cross, b_ff1, b_ff2, b_out]
        big = [latent.reshape(batch, blk, ch), context, w_in, w_self, w_cross_q, w_cross_kv, w_cross_o, w_ff1, w_ff2, w_out]
        out = pl.pallas_call(
            functools.partial(whole_kernel, n, per_chip, ch // NUM_GROUPS),
            out_shape=jax.ShapeDtypeStruct((batch, blk, ch), BF16),
            in_specs=[VMEM] * len(small) + [ANY] * len(big), out_specs=ANY, scratch_shapes=scratch,
            compiler_params=pltpu.CompilerParams(collective_id=0, has_side_effects=True, vmem_limit_bytes=62 * 1024 * 1024),
        )(*small, *big)
        return out.reshape(batch, rows, columns, ch)

    in_specs = (tok_spec, ctx_spec) + (replicated,) * 18
    return jax.shard_map(local_forward, mesh=mesh, in_specs=in_specs, out_specs=tok_spec, check_vma=False)
```

```python
import functools
import math

import jax
import jax.numpy as jnp
from jax import lax
from jax.experimental import pallas as pl
from jax.experimental.pallas import tpu as pltpu
from jax.sharding import PartitionSpec as P

HEAD_DIM = 64
NUM_GROUPS = 32
CORES = 2
TILE = 256
FF_CHUNK = 512
TEXT_PAD = 128
KEY_CHUNK = 512
LANES = 128
MESH = pl.DeviceIdType.MESH
F32 = jnp.float32
BF16 = jnp.bfloat16
ANY = pl.BlockSpec(memory_space=pl.ANY)
VMEM = pl.BlockSpec(memory_space=pltpu.VMEM)
NT = (((1,), (1,)), ((), ()))


def dot(a, b):
    return jnp.dot(a, b, preferred_element_type=F32)


def dot_nt(a, b):
    return lax.dot_general(a, b, NT, preferred_element_type=F32)


def layer_norm(hidden, gain, bias):
    vals = hidden.astype(F32)
    mean_val = jnp.mean(vals, axis=-1, keepdims=True)
    centered = vals - mean_val
    var_val = jnp.mean(centered * centered, axis=-1, keepdims=True)
    scaled = centered * lax.rsqrt(var_val + 1e-5)
    return (scaled * gain.astype(F32) + bias.astype(F32)).astype(BF16)


def entry_barrier(n):
    me = lax.axis_index('sp')
    sem = pltpu.get_barrier_semaphore()
    for k in range(1, n):
        pl.semaphore_signal(sem, inc=1, device_id={'sp': lax.rem(me + k, n)}, device_id_type=MESH)
    pl.semaphore_wait(sem, n - 1)


def group_sum(row, ind):
    hi = row.astype(BF16)
    rest = row - hi.astype(F32)
    mid = rest.astype(BF16)
    low = (rest - mid.astype(F32)).astype(BF16)
    total = None
    for piece in (low, mid, hi):
        term = dot(jnp.broadcast_to(piece, (16, piece.shape[1])), ind)[0:1]
        total = term if total is None else total + term
    return total


def same_group(ch, group_ch):
    def gid(axis):
        pos = lax.broadcasted_iota(jnp.int32, (ch, ch), axis).astype(F32)
        return jnp.floor((pos + 0.5) * (1.0 / group_ch))
    return jnp.where(gid(0) == gid(1), 1.0, 0.0).astype(BF16)


def column_stats(x_ref, lo, hi, count, ind):
    steps = (hi - lo) // TILE
    zero = jnp.zeros((1, x_ref.shape[1]), F32)

    def rows(i):
        return x_ref[pl.ds(pl.multiple_of(lo + i * TILE, TILE), TILE), :].astype(F32)

    mean = group_sum(lax.fori_loop(0, steps, lambda i, acc: acc + jnp.sum(rows(i), axis=0, keepdims=True), zero), ind) / count

    def sq(i, acc):
        d = rows(i) - mean
        return acc + jnp.sum(d * d, axis=0, keepdims=True)
    return mean, group_sum(lax.fori_loop(0, steps, sq, zero), ind)


def qkv_tile(hid, gain, bias, wqkv, slot, r0, k0, q_ref, k_ref, vt_ref):
    ch = hid.shape[1]
    a = layer_norm(hid, gain, bias)
    r = dot(a, wqkv[...]).astype(BF16)
    q_ref[pl.ds(r0, TILE), :] = r[:, :ch]
    k_ref[slot, pl.ds(k0, TILE), :] = r[:, ch:2 * ch]
    vt_ref[slot, :, pl.ds(k0, TILE)] = r[:, 2 * ch:].T


def head_mask(qp, half):
    lane = lax.broadcasted_iota(jnp.int32, qp.shape, 1)
    return jnp.where((lane >= HEAD_DIM) if half else (lane < HEAD_DIM), qp, jnp.zeros_like(qp))


def self_attend(slot, r0, q_ref, k_ref, vt_ref, s0, s1, ot, scale):
    keys, ch = k_ref.shape[1:]
    pairs = ch // LANES

    def step(cur, top, d0, nxt, pair, half):
        col = pl.multiple_of(pair * LANES, LANES)
        if nxt is not None:
            qm = head_mask(q_ref[pl.ds(r0, TILE), pl.ds(col, LANES)], half)
        new_top = total = acc = None
        for c in range(0, keys, KEY_CHUNK):
            rows = slice(c, c + KEY_CHUNK)
            if nxt is not None:
                s = dot_nt(k_ref[slot, rows, pl.ds(col, LANES)], qm)
                nxt[rows, :] = s
                peak = jnp.max(s, axis=0, keepdims=True)
                new_top = peak if new_top is None else jnp.maximum(new_top, peak)
            if cur is not None:
                p = jnp.exp2(cur[rows, :] * scale - top)
                part = jnp.sum(p, axis=0, keepdims=True)
                prod = dot(vt_ref[slot, pl.ds(d0, HEAD_DIM), rows], p.astype(BF16))
                total = part if total is None else total + part
                acc = prod if acc is None else acc + prod
        if cur is not None:
            ot[pl.ds(d0, HEAD_DIM), :] = (acc / total).astype(BF16)
        return None if nxt is None else new_top * scale

    def body(pair, top):
        d0 = pl.multiple_of(pair * LANES, LANES)
        top = step(s0, top, d0, s1, pair, 1)
        return step(s1, top, pl.multiple_of(d0 + HEAD_DIM, HEAD_DIM), s0, lax.rem(pair + 1, pairs), 0)

    lax.fori_loop(0, pairs, body, step(None, None, 0, s0, 0, 0))


def text_attend(layer, slot, qc, tk, tvt, ot, text_len, scale):
    ch = qc.shape[1]
    used = -(-text_len // 16) * 16
    heads = ch // HEAD_DIM
    scores = []
    for h in range(heads):
        cols = slice(h // 2 * LANES, (h // 2 + 1) * LANES)
        scores.append(dot_nt(tk[layer, slot, 0:used, cols], head_mask(qc[:, cols], h % 2)))
    keep = lax.broadcasted_iota(jnp.int32, scores[0].shape, 0) < text_len
    for h in range(heads):
        s = jnp.where(keep, scores[h], jnp.finfo(F32).min)
        top = jnp.max(s, axis=0, keepdims=True) * scale
        p = jnp.where(keep, jnp.exp2(s * scale - top), 0.0)
        total = jnp.sum(p, axis=0, keepdims=True)
        pb = jnp.concatenate([p.astype(BF16), jnp.zeros((TEXT_PAD - used, p.shape[1]), BF16)], axis=0)
        ot[h * HEAD_DIM:(h + 1) * HEAD_DIM, :] = (dot(tvt[layer, slot, h * HEAD_DIM:(h + 1) * HEAD_DIM, :], pb) / total).astype(BF16)


def whole_kernel(n, per_chip, group_ch,
                 gng_in, gnb_in, bin_in, lng_in, lnb_in, bself_in, bcross_in, bff1_in, bff2_in, bout_in,
                 x_ref, ctx_ref, win_ref, wself_ref, wcq_ref, wxkv_ref, wco_ref, wff1_ref, wff2_ref, wout_ref,
                 out_ref,
                 gng_ref, gnb_ref, bin_ref, lng_ref, lnb_ref, bself_ref, bcross_ref, bff1_ref, bff2_ref, bout_ref,
                 xs, hs, qs, k0, k1, vt0, vt1, s0, s1, ot, tk, tvt, vtmp, ctx, wx, win, wout, wo2, wcq2, wco2, wff12, wff22, wqkv0, wqkv1,
                 st_mine, st_peer, in_send, in_recv, out_send, out_recv, local_sem, st_sem, kv_send, kv_recv, w_sem, c_sem, x_sem, small_sem):
    me = lax.axis_index('sp')
    chip, core = me // CORES, lax.rem(me, CORES)
    peer = chip * CORES + (CORES - 1 - core)
    blk, ch = x_ref.shape[1:]
    part = blk // CORES
    own = n * blk
    rows = xs.shape[0]
    shared = rows - own
    ff = wff22.shape[1]
    text_len = ctx_ref.shape[1]
    own_tiles, sh_tiles = own // TILE, shared // TILE
    scale = HEAD_DIM ** -0.5 * math.log2(math.e)
    ks, vts, wqkvs = (k0, k1), (vt0, vt1), (wqkv0, wqkv1)
    layers = wself_ref.shape[0]

    ctx_loads = [pltpu.make_async_copy(ctx_ref.at[chip * per_chip + core], ctx.at[0], c_sem.at[0]),
                 pltpu.make_async_copy(ctx_ref.at[chip * per_chip + CORES], ctx.at[1], c_sem.at[1])]

    def text_loads(layer):
        return [pltpu.make_async_copy(wxkv_ref.at[layer, j], wx.at[j], x_sem.at[j]) for j in range(2)]

    def qkv_loads(layer):
        return [pltpu.make_async_copy(wself_ref.at[layer, j], wqkvs[layer].at[:, pl.ds(j * ch, ch)], w_sem.at[10 * layer + j]) for j in range(3)]

    def layer_loads(layer):
        pairs = ((wself_ref.at[layer, 3], wo2), (wcq_ref.at[layer], wcq2), (wco_ref.at[layer], wco2), (wff1_ref.at[layer], wff12), (wff2_ref.at[layer], wff22))
        return [pltpu.make_async_copy(src, dst.at[layer], w_sem.at[13 + 5 * layer + j]) for j, (src, dst) in enumerate(pairs)]

    edge_loads = [pltpu.make_async_copy(win_ref, win, w_sem.at[8]), pltpu.make_async_copy(wout_ref, wout, w_sem.at[9])]

    def begin(copies):
        for c in copies:
            c.start()

    def finish(copies):
        for c in copies:
            c.wait()

    def in_copy(i, src, dest):
        to_chip, to_core = dest // CORES, lax.rem(dest, CORES)
        source = (x_ref.at[to_chip * per_chip + to_core],
                  x_ref.at[to_chip * per_chip + CORES, pl.ds(pl.multiple_of(to_core * part, part), part)])[i]
        target = (xs.at[pl.ds(pl.multiple_of(src * blk, blk), blk)],
                  xs.at[pl.ds(pl.multiple_of(own + src * part, part), part)])[i]
        return source, target

    def in_remote(i, src, dest):
        source, target = in_copy(i, src, dest)
        return pltpu.make_async_remote_copy(
            src_ref=source, dst_ref=target, send_sem=in_send.at[i, dest], recv_sem=in_recv.at[i, src],
            device_id={'sp': dest}, device_id_type=MESH)

    def out_copy(i, src, dest):
        from_chip, from_core = src // CORES, lax.rem(src, CORES)
        source = (xs.at[pl.ds(pl.multiple_of(dest * blk, blk), blk)],
                  xs.at[pl.ds(pl.multiple_of(own + dest * part, part), part)])[i]
        target = (out_ref.at[from_chip * per_chip + from_core],
                  out_ref.at[from_chip * per_chip + CORES, pl.ds(pl.multiple_of(from_core * part, part), part)])[i]
        return source, target

    def out_remote(i, src, dest):
        source, target = out_copy(i, src, dest)
        return pltpu.make_async_remote_copy(
            src_ref=source, dst_ref=target, send_sem=out_send.at[i, dest], recv_sem=out_recv.at[i, src],
            device_id={'sp': dest}, device_id_type=MESH)

    def out_local(i):
        source, target = out_copy(i, me, me)
        return pltpu.make_async_copy(source, target, local_sem.at[2 + i])

    def send_out(i, dest):
        @pl.when(dest != me)
        def _():
            out_remote(i, me, dest).start()

        @pl.when(dest == me)
        def _():
            out_local(i).start()

    def kv_copies(layer):
        k, vt = ks[layer], vts[layer]
        args = ((k.at[1, pl.ds(0, shared)], k.at[1, pl.ds(shared, shared)]),
                (vt.at[1, :, pl.ds(0, shared)], vt.at[1, :, pl.ds(shared, shared)]))
        return [pltpu.make_async_remote_copy(
            src_ref=a, dst_ref=b, send_sem=kv_send.at[layer, j], recv_sem=kv_recv.at[layer, j],
            device_id={'sp': peer}, device_id_type=MESH) for j, (a, b) in enumerate(args)]

    begin(ctx_loads)
    begin(text_loads(0))
    locals_in = [pltpu.make_async_copy(*in_copy(i, me, me), local_sem.at[i]) for i in range(2)]
    begin(locals_in)
    entry_barrier(n)
    for k in range(1, n):
        in_remote(1, me, lax.rem(me + k, n)).start()
    small_loads = [pltpu.make_async_copy(src, dst, small_sem.at[j]) for j, (src, dst) in enumerate((
        (gng_in, gng_ref), (gnb_in, gnb_ref), (bin_in, bin_ref), (lng_in, lng_ref), (lnb_in, lnb_ref),
        (bself_in, bself_ref), (bcross_in, bcross_ref), (bff1_in, bff1_ref), (bff2_in, bff2_ref), (bout_in, bout_ref)))]
    begin(small_loads)
    begin(edge_loads)
    begin(qkv_loads(0))

    tk[...] = jnp.zeros_like(tk)
    vtmp[...] = jnp.zeros_like(vtmp)
    finish(ctx_loads)

    def text_keys(layer):
        finish(text_loads(layer))
        for s in range(2):
            tk[layer, s, 0:text_len, :] = dot(ctx[s], wx[0]).astype(BF16)
            vtmp[0:text_len, :] = dot(ctx[s], wx[1]).astype(BF16)
            tvt[layer, s] = vtmp[...].T

    text_keys(0)
    for k in range(1, n):
        in_remote(1, me, lax.rem(me + k, n)).wait_send()
    for k in range(1, n):
        in_remote(0, me, lax.rem(me + k, n)).start()
    begin(text_loads(1))
    begin(layer_loads(0))
    begin(qkv_loads(1))
    begin(layer_loads(1))
    ind = same_group(ch, group_ch)

    locals_in[1].wait()
    for k in range(1, n):
        in_remote(1, lax.rem(me + k, n), me).wait_recv()
    half = float(shared * group_ch)
    mean, m2 = column_stats(xs, own, rows, half, ind)
    st_mine[...] = jnp.zeros_like(st_mine)
    st_mine[0:1, :] = mean
    st_mine[1:2, :] = m2
    st_copy = pltpu.make_async_remote_copy(
        src_ref=st_mine, dst_ref=st_peer, send_sem=st_sem.at[0], recv_sem=st_sem.at[1], device_id={'sp': peer}, device_id_type=MESH)
    st_copy.start()
    finish(small_loads)
    finish(edge_loads)
    finish(qkv_loads(0))
    st_copy.wait()
    delta = mean - st_peer[0:1, :]
    mean_sh = (mean + st_peer[0:1, :]) * 0.5
    m2 = m2 + st_peer[1:2, :] + delta * delta * (half * 0.5)
    inv_sh = lax.rsqrt(m2 / (2.0 * half) + 1e-6)
    gain = gng_ref[...].astype(F32)[None, :]
    off = gnb_ref[...].astype(F32)[None, :]

    def enter(slot, mean, inv):
        def tile(i, carry):
            r0 = pl.multiple_of(slot * own + i * TILE, TILE)
            x = xs[pl.ds(r0, TILE), :].astype(F32)
            g = ((x - mean) * inv * gain + off).astype(BF16)
            hid = (dot(g, win[...]) + bin_ref[...].astype(F32)[None, :]).astype(BF16)
            hs[pl.ds(r0, TILE), :] = hid
            qkv_tile(hid, lng_ref[0, 0:1, :], lnb_ref[0, 0:1, :], wqkv0, slot, r0, pl.multiple_of(i * TILE, TILE), qs, k0, vt0)
            return carry
        return tile
    lax.fori_loop(0, sh_tiles, enter(1, mean_sh, inv_sh), 0)
    begin(kv_copies(0))
    text_keys(1)

    def own_entry():
        locals_in[0].wait()
        for k in range(1, n):
            in_remote(0, lax.rem(me + k, n), me).wait_recv()
        count = float(own * group_ch)
        mean, m2 = column_stats(xs, 0, own, count, ind)
        lax.fori_loop(0, own_tiles, enter(0, mean, lax.rsqrt(m2 / count + 1e-6)), 0)

    for layer in range(layers):
        last = layer == layers - 1
        k_all, vt_all = ks[layer], vts[layer]
        loads = layer_loads(layer)
        wo, wcq, wco, wff1, wff2 = (w.at[layer] for w in (wo2, wcq2, wco2, wff12, wff22))
        for c in kv_copies(layer):
            c.wait_recv()

        def tile(it, carry):
            f = (it + own_tiles - sh_tiles) // own_tiles
            slot = 1 - f
            idx = f * lax.rem(chip + 1 + it + own_tiles - sh_tiles, own_tiles) + slot * (own_tiles + it)
            r0 = pl.multiple_of(idx * TILE, TILE)
            k0r = pl.multiple_of(idx * TILE - slot * own, TILE)
            if layer == 0:
                pl.when(it == sh_tiles)(own_entry)
            self_attend(slot, r0, qs, k_all, vt_all, s0, s1, ot, scale)

            @pl.when(it == 0)
            def _():
                finish(loads)
                if not last:
                    finish(qkv_loads(layer + 1))
            hid = (hs[pl.ds(r0, TILE), :].astype(F32) + dot(ot[...].T, wo[...]) + bself_ref[layer:layer + 1, :].astype(F32)).astype(BF16)
            qc = dot(layer_norm(hid, lng_ref[1, layer:layer + 1, :], lnb_ref[1, layer:layer + 1, :]), wcq[...]).astype(BF16)
            text_attend(layer, slot, qc, tk, tvt, ot, text_len, scale)
            hid = (hid.astype(F32) + dot(ot[...].T, wco[...]) + bcross_ref[layer:layer + 1, :].astype(F32)).astype(BF16)
            a = layer_norm(hid, lng_ref[2, layer:layer + 1, :], lnb_ref[2, layer:layer + 1, :])
            acc = None
            for c0 in range(0, ff, FF_CHUNK):
                pc, qcol = slice(c0, c0 + FF_CHUNK), slice(ff + c0, ff + c0 + FF_CHUNK)
                p = (dot(a, wff1[:, pc]) + bff1_ref[layer:layer + 1, pc].astype(F32)).astype(BF16).astype(F32)
                g = (dot(a, wff1[:, qcol]) + bff1_ref[layer:layer + 1, qcol].astype(F32)).astype(BF16).astype(F32)
                z = (p * (0.5 * g * (1.0 + lax.erf(g * math.sqrt(0.5))))).astype(BF16)
                prod = dot(z, wff2[pc, :])
                acc = prod if acc is None else acc + prod
            hid = (hid.astype(F32) + acc + bff2_ref[layer:layer + 1, :].astype(F32)).astype(BF16)
            if last:
                y = dot(hid, wout[...]) + bout_ref[...].astype(F32)[None, :] + xs[pl.ds(r0, TILE), :].astype(F32)
                xs[pl.ds(r0, TILE), :] = y.astype(BF16)

                @pl.when(slot == 0)
                def _():
                    for j in range(TILE // blk):
                        send_out(0, idx * (TILE // blk) + j)

                @pl.when(slot == 1)
                def _():
                    for j in range(TILE // part):
                        send_out(1, (idx - own_tiles) * (TILE // part) + j)
            else:
                hs[pl.ds(r0, TILE), :] = hid
                qkv_tile(hid, lng_ref[0, layer + 1:layer + 2, :], lnb_ref[0, layer + 1:layer + 2, :], wqkvs[layer + 1], slot, r0, k0r, qs,
                         ks[layer + 1], vts[layer + 1])

                @pl.when(it == sh_tiles - 1)
                def _():
                    begin(kv_copies(layer + 1))
            return carry
        lax.fori_loop(0, own_tiles + sh_tiles, tile, 0)

    for layer in range(layers):
        for c in kv_copies(layer):
            c.wait_send()
    for i in range(2):
        out_local(i).wait()
        for k in range(1, n):
            other = lax.rem(me + k, n)
            if i == 0:
                in_remote(i, me, other).wait_send()
            out_remote(i, me, other).wait_send()
            out_remote(i, other, me).wait_recv()


def copy_kernel(src_ref, dst_ref, buf, sem):
    batch = src_ref.shape[0]
    loads = [pltpu.make_async_copy(src_ref.at[i], buf.at[i], sem.at[0, i]) for i in range(batch)]
    stores = [pltpu.make_async_copy(buf.at[i], dst_ref.at[i], sem.at[1, i]) for i in range(batch)]
    for c in loads:
        c.start()
    for a, b in zip(loads, stores):
        a.wait()
        b.start()
    for c in stores:
        c.wait()


def solution(mesh):
    n = mesh.shape['sp']
    tok_spec = P('dp', 'sp', None, None)
    ctx_spec = P('dp', None, None)
    replicated = P()
    dma = pltpu.SemaphoreType.DMA

    def local_forward(latent, context, gn_gain, gn_bias, w_in, b_in, ln_gain, ln_bias, w_self, b_self, w_cross_q, w_cross_kv, w_cross_o, b_cross, w_ff1, b_ff1, w_ff2, b_ff2, w_out, b_out):
        batch, rows, columns, ch = latent.shape
        blk = rows * columns
        ff = w_ff2.shape[1]
        layers, text_len, text_dim = w_self.shape[0], context.shape[1], context.shape[2]
        per_chip = batch * CORES // n
        assert per_chip == CORES + 1 and layers == 2
        own = n * blk
        toks = own + own // CORES

        def vm(*dims, dtype=BF16):
            return pltpu.VMEM(dims, dtype)

        scratch = [
            vm(toks, ch), vm(toks, ch), vm(toks, ch), vm(2, own, ch), vm(2, own, ch), vm(2, ch, own), vm(2, ch, own),
            vm(own, TILE, dtype=F32), vm(own, TILE, dtype=F32), vm(ch, TILE),
            vm(layers, 2, TEXT_PAD, ch), vm(layers, 2, ch, TEXT_PAD), vm(TEXT_PAD, ch), vm(2, text_len, text_dim), vm(2, text_dim, ch),
            vm(ch, ch), vm(ch, ch), vm(layers, ch, ch), vm(layers, ch, ch), vm(layers, ch, ch), vm(layers, ch, 2 * ff), vm(layers, ff, ch), vm(ch, 3 * ch), vm(ch, 3 * ch),
            vm(32, ch, dtype=F32), vm(32, ch, dtype=F32),
            dma((2, n)), dma((2, n)), dma((2, n)), dma((2, n)), dma((4,)), dma((2,)), dma((layers, 2)), dma((layers, 2)), dma((23,)), dma((2,)), dma((2,))]
        small = [gn_gain, gn_bias, b_in, ln_gain.transpose(1, 0, 2), ln_bias.transpose(1, 0, 2), b_self, b_cross, b_ff1, b_ff2, b_out]
        big = [latent.reshape(batch, blk, ch), context, w_in, w_self, w_cross_q, w_cross_kv, w_cross_o, w_ff1, w_ff2, w_out]
        scratch = [pltpu.VMEM(a.shape, a.dtype) for a in small] + scratch + [dma((len(small),))]
        out = pl.pallas_call(
            functools.partial(whole_kernel, n, per_chip, ch // NUM_GROUPS),
            out_shape=jax.ShapeDtypeStruct((batch, blk, ch), BF16),
            in_specs=[ANY] * (len(small) + len(big)), out_specs=ANY, scratch_shapes=scratch,
            compiler_params=pltpu.CompilerParams(collective_id=0, has_side_effects=True, vmem_limit_bytes=62 * 1024 * 1024),
        )(*small, *big)
        out = pl.pallas_call(
            copy_kernel, out_shape=jax.ShapeDtypeStruct(out.shape, BF16), in_specs=[ANY], out_specs=ANY,
            scratch_shapes=[vm(*out.shape), dma((2, batch))],
        )(out)
        return out.reshape(batch, rows, columns, ch)

    in_specs = (tok_spec, ctx_spec) + (replicated,) * 18
    return jax.shard_map(local_forward, mesh=mesh, in_specs=in_specs, out_specs=tok_spec, check_vma=False)
```
